32 devices in a mesh: seq: 8 (over z, core), tp: 4 (over y, x).
Axes of the slice: x: 2, y: 2, z: 4, core: 2. Of those that a mesh axis runs over, the one named last changes fastest.
Arguments:
- hidden_in: bfloat16 [4096, 4608], P('seq'), may hold values from -6 to 6
- pre_gain: float32 [4608], replicated, may hold values from 0.5 to 1.5
- w_query: bfloat16 [4608, 4096], P(None, 'tp'), may hold values from -0.09375 to 0.09375
- key_cache: bfloat16 [8192, 2048], P('seq', 'tp'), may hold values from -12 to 12
- value_cache: bfloat16 [8192, 2048], P('seq', 'tp'), may hold values from -6 to 6
- w_out: bfloat16 [4096, 4608], P('tp'), may hold values from -0.75 to 0.75
- post_gain: float32 [4608], replicated, may hold values from 0.5 to 1.5
- starts: int32 [8], replicated, may hold values from 0 to 7680, as said below
- counts: int32 [8], replicated, may hold values from 512 to 1024, as said below
Outputs:
- layer_out: bfloat16 [4096, 4608], P(('seq', 'tp'))
The draws below stay inside these ranges and needn't reach their ends.
Inputs may be any that keep to these rules, and one draw needn't show every extreme that they name: The queries of shard s sit at positions starts[s] to starts[s] + 511, all inside the filled rows of shard s, that is from s * 1024 to s * 1024 + counts[s] - 1. `counts`: at least one shard is full.
All inputs are finite; a program needn't handle non-finite values.
Results may differ from the reference program's by a relative error of at most 0.012.
Values may be sent and summed in bfloat16 or wider, within the bound.
A program may use at most 128 MiB of HBM per device.

```python
import jax
import jax.numpy as jnp
from jax import lax

D = 4608
H = 32
KVH = 16
HD = 128
WINDOW = 4096
CTX_DEV = 1024
Q_DEV = 512
HALO = 4
CONTEXT = 8192
TOKENS = 4096
N_SEQ = 8
N_TP = 4


def fill_table(key):
    count_key = jax.random.fold_in(key, 11)
    full_key = jax.random.fold_in(key, 12)
    offset_key = jax.random.fold_in(key, 13)
    shard_ids = jnp.arange(N_SEQ, dtype=jnp.int32)
    counts = jax.random.randint(count_key, (N_SEQ,), Q_DEV, CTX_DEV + 1, dtype=jnp.int32)
    full_shard = jax.random.randint(full_key, (), 0, N_SEQ, dtype=jnp.int32)
    counts = jnp.where(shard_ids == full_shard, jnp.int32(CTX_DEV), counts)
    offsets = jax.random.randint(offset_key, (N_SEQ,), 0, counts - Q_DEV + 1, dtype=jnp.int32)
    starts = shard_ids * CTX_DEV + offsets
    return (starts.astype(jnp.int32), counts.astype(jnp.int32))


def draw_starts(key, part):
    return fill_table(key)[0]


def draw_counts(key, part):
    return fill_table(key)[1]


def levels(rng, shape, shards, least, top_value):
    def one(axis_at, blocks):
        draws = jax.random.uniform(jax.random.fold_in(jax.random.fold_in(rng, 6), axis_at), (blocks,), jnp.float32, least / len(shards), top_value / len(shards))
        return jnp.repeat(jnp.exp(draws), shape[axis_at] // blocks).reshape((-1,) + (1,) * (len(shape) - axis_at - 1))

    level = one(*shards[0])
    for cut in shards[1:]:
        level = level * one(*cut)
    return level


def gaussian(key, shape, scale, reach, shards=(), kind=jnp.bfloat16):
    gain = levels(key, shape, shards, -0.22, 0.18) if shards else 1.0
    result = jax.random.normal(key, shape, jnp.float32) * scale * gain
    return jnp.minimum(jnp.maximum(result, -reach), reach).astype(kind)


def setup_inputs(seed: int = 0) -> dict:
    seeds = jax.random.split(jax.random.key(seed), 10)
    hidden_in = gaussian(seeds[0], (TOKENS, D), 1.0, 6.0, ((0, 8),))
    pre_gain = jnp.clip(1.0 + 0.1 * jax.random.normal(seeds[1], (D,), jnp.float32), 0.5, 1.5)
    w_query = gaussian(seeds[2], (D, H * HD), D ** -0.5, 0.09375, ((1, 4),))
    key_cache = gaussian(seeds[3], (CONTEXT, KVH * HD), 2.0, 12.0, ((0, 8), (1, 4)))
    value_cache = gaussian(seeds[4], (CONTEXT, KVH * HD), 1.0, 6.0, ((0, 8), (1, 4)))
    w_out = gaussian(seeds[5], (H * HD, D), (H * HD // 64) ** -0.5, 0.75, ((0, 4),))
    post_gain = jnp.clip(1.0 + 0.1 * jax.random.normal(seeds[6], (D,), jnp.float32), 0.5, 1.5)
    starts = draw_starts(jax.random.fold_in(seeds[9], 71), 0)
    counts = draw_counts(jax.random.fold_in(seeds[9], 71), 0)
    return dict(hidden_in=hidden_in, pre_gain=pre_gain, w_query=w_query, key_cache=key_cache, value_cache=value_cache, w_out=w_out, post_gain=post_gain, starts=starts, counts=counts)


def reference(hidden_in, pre_gain, w_query, key_cache, value_cache, w_out, post_gain, starts, counts):
    per_group = H // KVH
    key_span = (HALO + 1) * CTX_DEV
    inputs = hidden_in.astype(jnp.float32)
    normed = (inputs * lax.rsqrt(lax.optimization_barrier(jnp.mean(inputs * inputs, axis=-1, keepdims=True)) + 0.1) * pre_gain).astype(jnp.bfloat16)
    queries = (jnp.dot(normed, w_query, preferred_element_type=jnp.float32) * (D // H) ** (-0.5)).astype(jnp.bfloat16)
    padding = jnp.zeros((HALO * CTX_DEV, KVH * HD), jnp.bfloat16)
    keys_padded = jnp.concatenate([padding, key_cache], axis=0)
    values_padded = jnp.concatenate([padding, value_cache], axis=0)
    w_groups = w_out.astype(jnp.float32).reshape(N_TP, H * HD // N_TP, D)

    def one_shard(shard):
        shard = shard.astype(jnp.int32)
        query_block = lax.dynamic_slice_in_dim(queries, (shard * Q_DEV).astype(jnp.int32), Q_DEV, 0)
        key_block = lax.dynamic_slice_in_dim(keys_padded, (shard * CTX_DEV).astype(jnp.int32), key_span, 0)
        value_block = lax.dynamic_slice_in_dim(values_padded, (shard * CTX_DEV).astype(jnp.int32), key_span, 0)
        key_pos = (shard - HALO) * CTX_DEV + jnp.arange(key_span, dtype=jnp.int32)
        source = jnp.clip(key_pos // CTX_DEV, 0, N_SEQ - 1).astype(jnp.int32)
        filled = (key_pos >= 0) & (key_pos - source * CTX_DEV < counts[source])
        query_pos = starts[shard] + jnp.arange(Q_DEV, dtype=jnp.int32)
        allowed = filled[None, :] & (key_pos[None, :] <= query_pos[:, None]) & (key_pos[None, :] > query_pos[:, None] - WINDOW)
        query_f = lax.optimization_barrier(query_block).astype(jnp.float32).reshape(Q_DEV, KVH, per_group, HD)
        key_f = key_block.astype(jnp.float32).reshape(key_span, KVH, HD)
        value_f = value_block.astype(jnp.float32).reshape(key_span, KVH, HD)
        scores = jnp.einsum('qkgd,ckd->kgqc', query_f, key_f, precision=lax.Precision.HIGHEST)
        scores = 50.0 * jnp.tanh(scores / 50.0)
        weight = jnp.where(allowed[None, None], jnp.exp(scores), jnp.float32(0.0))
        denominator = lax.optimization_barrier(jnp.sum(weight, axis=-1))
        weight16 = lax.optimization_barrier(weight.astype(jnp.bfloat16)).astype(jnp.float32)
        context = jnp.einsum('kgqc,ckd->qkgd', weight16, value_f, precision=lax.Precision.HIGHEST)
        attended = (context / jnp.transpose(denominator, (2, 0, 1))[..., None]).reshape(Q_DEV, H * HD).astype(jnp.bfloat16)
        attended_f = lax.optimization_barrier(attended).astype(jnp.float32).reshape(Q_DEV, N_TP, H * HD // N_TP)
        partial_value = jnp.einsum('qtf,tfd->tqd', attended_f, w_groups, precision=lax.Precision.HIGHEST)
        partial_value = lax.optimization_barrier(partial_value.astype(jnp.bfloat16)).astype(jnp.float32)
        projected = lax.optimization_barrier(jnp.sum(partial_value, axis=0))
        residual = lax.dynamic_slice_in_dim(hidden_in, (shard * Q_DEV).astype(jnp.int32), Q_DEV, 0).astype(jnp.float32)
        mixed = residual + projected * lax.rsqrt(lax.optimization_barrier(jnp.mean(projected * projected, axis=-1, keepdims=True)) + 0.1) * post_gain
        return mixed.astype(jnp.bfloat16)
    layer_out = lax.map(one_shard, jnp.arange(N_SEQ, dtype=jnp.int32))
    return layer_out.reshape(N_SEQ * Q_DEV, D)
```

```python
import functools
import math

import jax
import jax.numpy as jnp
from jax import lax
from jax.experimental import pallas as pl
from jax.experimental.pallas import tpu as pltpu
from jax.sharding import PartitionSpec as P

HEADS = 32
HD = 128
WINDOW = 4096
SUB = 16
G = 2
KB = 256
KT = 512
NT = 2304
SOFT = 50.0
GAIN = SOFT * math.log2(math.e)
MESH = pl.DeviceIdType.MESH
F32 = jnp.float32
BF16 = jnp.bfloat16


def kernel(
    n, n_tp, kvh, NC,
    starts, counts, hidden, pre_gain, wq, key, value, wout, post_gain, out,
    hbuf, wqb, wob, kraw, kt, vb, q0, q2, q4, fs, fr, ns, nr, acc, accd, num, den, rel, sc0, sc1, pw0, pw1,
    proj, ra1, pa, ra2, rb1, pb, rb2, res, obuf, att,
    hsem, wqsem, wosem, kvsem, ressem, osem,
    s1, r1, sn, rn, sf, rf, sF, rF, sN, rN,
    sa1, ta1, sa2, ta2, sb1, tb1, sb2, tb2,
):
    sc = (sc0, sc1)
    pw = (pw0, pw1)
    s = lax.axis_index("seq")
    t = lax.axis_index("tp")
    odd = lax.rem(s, 2)
    partner = s + 1 - 2 * odd
    rows, d = hidden.shape
    ctx = key.shape[0]
    sub = rows // (NC * n_tp)
    chunk = rows // NC
    tall = 2 * chunk
    owned = rows // n_tp
    NF = NC // G
    has_prev = s >= 2
    has_next = s + 2 < n
    has_far = s + 4 < n

    def h_copy(c, b):
        return pltpu.make_async_copy(
            hidden.at[pl.ds(pl.multiple_of(b * owned + c * sub, sub), sub)], hbuf.at[c, b], hsem.at[c, b])

    def wq_copy(h):
        return pltpu.make_async_copy(
            wq.at[:, pl.ds(pl.multiple_of(h * 2 * HD, 2 * HD), 2 * HD)], wqb.at[h], wqsem.at[h])

    def cols(h):
        return pl.ds(pl.multiple_of(h * HD, HD), HD)

    def kv_local(h):
        return [
            pltpu.make_async_copy(src.at[:, cols(h)], dst.at[0, h], kvsem.at[h, j])
            for j, (src, dst) in enumerate(((key, kraw), (value, vb)))
        ]

    for c in range(NC // 2):
        for b in range(n_tp):
            h_copy(c, b).start()
    for h in range(kvh):
        wq_copy(h).start()
    for c in range(NC // 2, NC):
        for b in range(n_tp):
            h_copy(c, b).start()
    for h in range(kvh):
        for cp in kv_local(h):
            cp.start()

    barrier = pltpu.get_barrier_semaphore()
    pl.semaphore_signal(barrier, inc=1, device_id=(partner, t), device_id_type=MESH)
    for k in range(1, n_tp):
        pl.semaphore_signal(barrier, inc=1, device_id=(s, lax.rem(t + k, n_tp)), device_id_type=MESH)

    @pl.when(has_prev)
    def _():
        pl.semaphore_signal(barrier, inc=1, device_id=(s - 2, t), device_id_type=MESH)

    @pl.when(has_next)
    def _():
        pl.semaphore_signal(barrier, inc=1, device_id=(s + 2, t), device_id_type=MESH)

    pl.semaphore_wait(
        barrier, n_tp + jnp.where(has_prev, 1, 0) + jnp.where(has_next, 1, 0))

    def kv_partner(h):
        return [
            pltpu.make_async_remote_copy(
                src.at[:, cols(h)], dst.at[1, h], s1.at[h, j], r1.at[h, j],
                device_id=(partner, t), device_id_type=MESH)
            for j, (src, dst) in enumerate(((key, kraw), (value, vb)))
        ]

    def along(src, dst, send, recv, to):
        def make(c):
            return pltpu.make_async_remote_copy(
                src.at[c], dst.at[c], send.at[c], recv.at[c],
                device_id=(to, t), device_id_type=MESH)
        return make

    q_near = along(q0, q2, sn, rn, s - 2)
    q_far = along(q2, q4, sf, rf, s - 2)
    p_far = along(fs, fr, sF, rF, s + 2)
    p_near = along(ns, nr, sN, rN, s + 2)

    nx = 2
    ny = n_tp // nx
    half = d // 2
    x_own = lax.rem(t, nx)
    y_own = lax.div(t, nx)
    left = pl.ds(0, half)
    right = pl.ds(half, half)

    def remote(src, dst, send, recv, to):
        return pltpu.make_async_remote_copy(
            src, dst, send, recv, device_id=(s, to), device_id_type=MESH)

    def first_phase(c):
        copies = []
        for k in range(1, nx):
            xt = lax.rem(x_own + k, nx)
            copies.append(remote(
                proj.at[c, :, xt, :, :, left], ra1.at[c, k - 1], sa1.at[c, k - 1], ta1.at[c, k - 1],
                y_own * nx + xt))
        for k in range(1, ny):
            yt = lax.rem(y_own + k, ny)
            copies.append(remote(
                proj.at[c, yt, :, :, :, right], rb1.at[c, k - 1], sb1.at[c, k - 1], tb1.at[c, k - 1],
                yt * nx + x_own))
        return copies

    def second_phase(c):
        copies = []
        for k in range(1, ny):
            yt = lax.rem(y_own + k, ny)
            copies.append(remote(
                pa.at[c, yt], ra2.at[c, k - 1], sa2.at[c, k - 1], ta2.at[c, k - 1],
                yt * nx + x_own))
        for k in range(1, nx):
            xt = lax.rem(x_own + k, nx)
            copies.append(remote(
                pb.at[c, xt], rb2.at[c, k - 1], sb2.at[c, k - 1], tb2.at[c, k - 1],
                y_own * nx + xt))
        return copies

    for h in range(kvh):
        for cp in kv_partner(h):
            cp.start()
    wo_copy = pltpu.make_async_copy(wout, wob, wosem)
    wo_copy.start()
    res_copy = pltpu.make_async_copy(
        hidden.at[pl.ds(pl.multiple_of(t * owned, owned), owned)], res, ressem)
    res_copy.start()

    shape = (2, n_tp, sub, KB)
    rel[...] = (
        lax.broadcasted_iota(jnp.int32, shape, 3)
        - lax.broadcasted_iota(jnp.int32, shape, 1) * owned
        - lax.broadcasted_iota(jnp.int32, shape, 2)
    ).reshape(tall, KB)

    @pl.when(s < 2)
    def _():
        fr[...] = jnp.zeros_like(fr)
        nr[...] = jnp.zeros_like(nr)

    def queries(c0, count):
        def norm(i, carry):
            c = c0 + i // n_tp
            b = i % n_tp
            h_copy(c, b).wait()
            x = hbuf[c, b].astype(F32)
            y = x * lax.rsqrt(jnp.mean(x * x, axis=-1, keepdims=True) + 0.1) * pre_gain[...]
            hbuf[c, b] = y.astype(BF16)
            return carry

        lax.fori_loop(0, count * n_tp, norm, 0, unroll=4)

        def project(h, carry):
            if c0 == 0:
                wq_copy(h).wait()
            x = hbuf[c0:c0 + count].reshape(count * chunk, d)
            y = jnp.dot(x, wqb[h], preferred_element_type=F32) * ((d // HEADS) ** -0.5 / SOFT)
            y = y.astype(BF16)
            for i in range(count):
                q0[c0 + i, h, 0:chunk] = y[i * chunk:(i + 1) * chunk, :HD]
                q0[c0 + i, h, chunk:tall] = y[i * chunk:(i + 1) * chunk, HD:]
            return carry

        lax.fori_loop(0, kvh, project, 0)

    queries(0, NC // 2)

    @pl.when(has_prev)
    def _():
        q_near(0).start()
        q_near(1).start()

    queries(NC // 2, NC // 2)

    def turn(src):
        def body(h, carry):
            for cp in (kv_local(h) if src == 0 else kv_partner(h)):
                if src == 0:
                    cp.wait()
                else:
                    cp.wait_recv()
            kt[src, h] = kraw[src, h].T
            return carry

        lax.fori_loop(0, kvh, body, 0)

    turn(0)
    turn(1)

    off_own = starts[s] - s * ctx
    s_far = jnp.minimum(s + 4, n - 1)
    off_far = starts[s_far] - s_far * ctx + 4 * ctx - WINDOW
    fill0 = counts[s]
    fill1 = counts[partner]
    lane = lax.broadcasted_iota(jnp.int32, (1, KB), 1)

    def unit(q, c, sources, num, den):
        tiles = [
            (h, src, mode, i)
            for h in range(kvh) for src, mode in sources for i in range(ctx // KT)
        ]
        last = len(sources) * (ctx // KT)
        tops = {}
        belows = {}

        def scores(j):
            h, src, mode, i = tiles[j]
            qt = q[c, h]
            for b in range(0, KT, KB):
                at = i * KT + b
                sc[j % 2][:, b:b + KB] = jnp.dot(
                    qt, kt[src, h, :, at:at + KB], preferred_element_type=F32)

        def weights(j):
            h, src, mode, i = tiles[j]
            fill = fill1 if src else fill0
            below = belows.get(h)
            for b in range(0, KT, KB):
                at = i * KT + b
                p = jnp.exp2(jnp.tanh(sc[j % 2][:, b:b + KB]) * GAIN)
                if mode == 1:
                    p = jnp.where(rel[...] <= off_own + c * sub - at, p, 0.0)
                elif mode == 2:
                    ok = (rel[...] > off_far + c * sub - at) & (lane < fill - at)
                    p = jnp.where(ok, p, 0.0)
                else:
                    p = jnp.where(lane < fill - at, p, 0.0)
                for k in range(0, KB, HD):
                    part = p[:, k:k + HD]
                    below = part if below is None else below + part
                pw[j % 2][:, b:b + KB] = p.astype(BF16)
            belows[h] = below
            if j % last == last - 1:
                den[h] = below

        def values(j):
            h, src, mode, i = tiles[j]
            a = jnp.dot(
                pw[j % 2][...], vb[src, h, i * KT:(i + 1) * KT], preferred_element_type=F32)
            tops[h] = tops[h] + a if h in tops else a
            if j % last == last - 1:
                num[h] = tops[h]

        count = len(tiles)
        for k in range(count + 2):
            if k < count:
                scores(k)
            if 0 <= k - 1 < count:
                weights(k - 1)
            if 0 <= k - 2:
                values(k - 2)

    blocks = tall // HD
    lanes = lax.broadcasted_iota(jnp.int32, (tall, HD), 1)

    def received(src, c):
        parts = []
        for i in range(blocks):
            at = kvh * tall + 16 * i
            pair = src[c, at:at + 16].astype(F32)
            parts.append(pair[0:8] + pair[8:16])
        return parts[0] if blocks == 1 else jnp.concatenate(parts, axis=1)

    def emit(c, dst, extra):
        pack = jnp.zeros((tall, HD), F32)
        for h in range(kvh):
            pack = jnp.where(lanes == h, jnp.sum(den[h], axis=-1, keepdims=True), pack)
        dens = pack.T[0:8]
        if extra is not None:
            dens += received(extra, c)
        hi = dens.astype(BF16).astype(F32)
        both = jnp.concatenate([hi, dens - hi], axis=0).astype(BF16)
        for i in range(blocks):
            at = kvh * tall + 16 * i
            dst[c, at:at + 16] = both[:, i * HD:(i + 1) * HD]
        for h in range(kvh):
            x = num[h]
            if extra is not None:
                x += extra[c, h * tall:(h + 1) * tall].astype(F32)
            dst[c, h * tall:(h + 1) * tall] = x.astype(BF16)

    def relay(c):
        @pl.when(has_next)
        def _():
            q_near(c).wait_recv()

        @pl.when(has_next & has_prev)
        def _():
            q_far(c).start()

    def far(c):
        q_far(c).wait_recv()

        @pl.when(odd == 0)
        def _():
            unit(q4, c, [(0, 2), (1, 0)], num, den)

        @pl.when(odd == 1)
        def _():
            unit(q4, c, [(0, 2)], num, den)

        emit(c, fs, None)
        p_far(c).start()

    def near(c):
        unit(q2, c, [(0, 0), (1, 0)], num, den)

        @pl.when(has_prev)
        def _():
            p_far(c).wait_recv()

        emit(c, ns, fr)
        p_near(c).start()

    def own(c):
        @pl.when(odd == 0)
        def _():
            unit(q0, c, [(0, 1)], acc.at[c], accd.at[c])

        @pl.when(odd == 1)
        def _():
            unit(q0, c, [(0, 1), (1, 0)], acc.at[c], accd.at[c])

    def finish(f):
        for z in range(G):
            c = f * G + z

            @pl.when(has_prev)
            def _():
                p_near(c).wait_recv()

            dens = received(nr, c)
            dens = jnp.concatenate([dens, jnp.zeros((HD - 8, tall), F32)], axis=0).T
            for h in range(kvh):
                total = jnp.sum(accd[c, h], axis=-1, keepdims=True) + dens[:, h:h + 1]
                top = acc[c, h] + nr[c, h * tall:(h + 1) * tall].astype(F32)
                a = (top * (1.0 / total)).astype(BF16)
                for g in range(2):
                    at = (2 * h + g) * HD
                    att[z * chunk:(z + 1) * chunk, at:at + HD] = a[g * chunk:(g + 1) * chunk]

        def column(i, inner):
            cs = pl.ds(pl.multiple_of(i * NT, NT), NT)
            y = jnp.dot(att[...], wob[:, cs], preferred_element_type=F32).astype(BF16)
            for z in range(G):
                proj[f, :, :, z, :, cs] = y[z * chunk:(z + 1) * chunk].reshape(ny, nx, sub, NT)
            return inner

        lax.fori_loop(0, d // NT, column, 0)
        for cp in first_phase(f):
            cp.start()

    def middle(c):
        for cp in first_phase(c):
            cp.wait_recv()
        for y in range(ny):
            part = proj[c, y, x_own, :, :, 0:half].astype(F32)
            for k in range(1, nx):
                part += ra1[c, k - 1, y].astype(F32)
            pa[c, y] = part.astype(BF16)
        for x in range(nx):
            part = proj[c, y_own, x, :, :, half:d].astype(F32)
            for k in range(1, ny):
                part += rb1[c, k - 1, x].astype(F32)
            pb[c, x] = part.astype(BF16)
        for cp in second_phase(c):
            cp.start()

    def out_copy(c):
        return pltpu.make_async_copy(
            obuf.at[c], out.at[pl.ds(pl.multiple_of(c * G * sub, G * sub), G * sub)], osem.at[c])

    def close(c):
        for cp in second_phase(c):
            cp.wait_recv()
        lo = pa[c, y_own].astype(F32)
        for k in range(1, ny):
            lo += ra2[c, k - 1].astype(F32)
        hi = pb[c, x_own].astype(F32)
        for k in range(1, nx):
            hi += rb2[c, k - 1].astype(F32)
        lo = lo.reshape(G * sub, half)
        hi = hi.reshape(G * sub, half)
        squares = jnp.sum(lo * lo, axis=-1, keepdims=True) + jnp.sum(hi * hi, axis=-1, keepdims=True)
        scale = lax.rsqrt(squares / d + 0.1)
        span = pl.ds(pl.multiple_of(c * G * sub, G * sub), G * sub)
        for v, at in ((lo, slice(0, half)), (hi, slice(half, d))):
            r = res[span, at].astype(F32)
            obuf[c, :, at] = (r + v * scale * post_gain[:, at]).astype(BF16)
        out_copy(c).start()

    wo_copy.wait()
    res_copy.wait()

    def step(k, carry):
        @pl.when(k < NC)
        def _():
            relay(k)

        @pl.when(has_prev & (k + 2 < NC))
        def _():
            q_near(k + 2).start()

        @pl.when(has_far & (k >= 1) & (k <= NC))
        def _():
            far(k - 1)

        @pl.when(has_next & (k >= 2) & (k <= NC + 1))
        def _():
            near(k - 2)

        @pl.when(k < NC)
        def _():
            own(k)

        even = lax.rem(k, G) == 0

        @pl.when(even & (k >= G + 2))
        def _():
            finish((k - 2 - G) // G)

        @pl.when((lax.rem(k, G) == G - 1) & (k >= 2 * G + 1))
        def _():
            middle((k - 2 * G - 1) // G)

        @pl.when((lax.rem(k, G) == G - 1) & (k >= 3 * G + 1))
        def _():
            close((k - 3 * G - 1) // G)

        return carry

    lax.fori_loop(0, NC + 3, step, 0)
    close(NF - 2)
    middle(NF - 1)
    close(NF - 1)

    def drain(h, carry):
        for cp in kv_partner(h):
            cp.wait_send()
        return carry

    lax.fori_loop(0, kvh, drain, 0)

    def drain_chunks(c, carry):
        @pl.when(has_prev)
        def _():
            q_near(c).wait_send()

        @pl.when(has_next & has_prev)
        def _():
            q_far(c).wait_send()

        @pl.when(has_far)
        def _():
            p_far(c).wait_send()

        @pl.when(has_next)
        def _():
            p_near(c).wait_send()

        return carry

    lax.fori_loop(0, NC, drain_chunks, 0)

    def drain_out(c, carry):
        for cp in first_phase(c) + second_phase(c):
            cp.wait_send()
        out_copy(c).wait()
        return carry

    lax.fori_loop(0, NF, drain_out, 0)


def shards(n, n_tp, hidden_in, pre_gain, w_query, key_cache, value_cache, w_out, post_gain, starts, counts):
    rows, d = hidden_in.shape
    ctx, kvw = key_cache.shape
    kvh = kvw // HD
    sub = SUB
    NC = rows // (n_tp * sub)
    NF = NC // G
    chunk = rows // NC
    tall = 2 * chunk
    nx, ny, half = 2, n_tp // 2, d // 2
    dma = pltpu.SemaphoreType.DMA
    kv = pltpu.VMEM((2, kvh, ctx, HD), BF16)
    queries = pltpu.VMEM((NC, kvh, tall, HD), BF16)
    partial = pltpu.VMEM((NC, kvh * tall + 16 * (tall // HD), HD), BF16)
    any_spec = pl.BlockSpec(memory_space=pl.ANY)
    vmem_spec = pl.BlockSpec(memory_space=pltpu.VMEM)
    smem_spec = pl.BlockSpec(memory_space=pltpu.SMEM)
    return pl.pallas_call(
        functools.partial(kernel, n, n_tp, kvh, NC),
        out_shape=jax.ShapeDtypeStruct((rows // n_tp, d), BF16),
        in_specs=[smem_spec, smem_spec, any_spec, vmem_spec] + [any_spec] * 4 + [vmem_spec],
        out_specs=any_spec,
        scratch_shapes=[
            pltpu.VMEM((NC, n_tp, sub, d), BF16),
            pltpu.VMEM((kvh, d, 2 * HD), BF16),
            pltpu.VMEM(w_out.shape, BF16),
            kv,
            pltpu.VMEM((2, kvh, HD, ctx), BF16),
            kv,
            queries, queries, queries,
            partial, partial, partial, partial,
            pltpu.VMEM((NC, kvh, tall, HD), F32),
            pltpu.VMEM((NC, kvh, tall, HD), F32),
            pltpu.VMEM((kvh, tall, HD), F32),
            pltpu.VMEM((kvh, tall, HD), F32),
            pltpu.VMEM((tall, KB), jnp.int32),
            pltpu.VMEM((tall, KT), F32), pltpu.VMEM((tall, KT), F32),
            pltpu.VMEM((tall, KT), BF16), pltpu.VMEM((tall, KT), BF16),
            pltpu.VMEM((NF, ny, nx, G, sub, d), BF16),
            pltpu.VMEM((NF, nx - 1, ny, G, sub, half), BF16),
            pltpu.VMEM((NF, ny, G, sub, half), BF16),
            pltpu.VMEM((NF, ny - 1, G, sub, half), BF16),
            pltpu.VMEM((NF, ny - 1, nx, G, sub, half), BF16),
            pltpu.VMEM((NF, nx, G, sub, half), BF16),
            pltpu.VMEM((NF, nx - 1, G, sub, half), BF16),
            pltpu.VMEM((rows // n_tp, d), BF16),
            pltpu.VMEM((NF, G * sub, d), BF16),
            pltpu.VMEM((G * chunk, w_out.shape[0]), BF16),
            dma((NC, n_tp)), dma((kvh,)), dma, dma((kvh, 2)), dma, dma((NF,)),
            dma((kvh, 2)), dma((kvh, 2)),
            dma((NC,)), dma((NC,)), dma((NC,)), dma((NC,)),
            dma((NC,)), dma((NC,)), dma((NC,)), dma((NC,)),
            dma((NF, nx - 1)), dma((NF, nx - 1)), dma((NF, ny - 1)), dma((NF, ny - 1)),
            dma((NF, ny - 1)), dma((NF, ny - 1)), dma((NF, nx - 1)), dma((NF, nx - 1)),
        ],
        compiler_params=pltpu.CompilerParams(
            collective_id=0, has_side_effects=True, vmem_limit_bytes=67_000_000),
        name="attention_block",
    )(starts, counts, hidden_in, pre_gain.reshape(1, d), w_query, key_cache, value_cache, w_out,
      post_gain.reshape(1, d))


def solution(mesh):
    return jax.shard_map(
        functools.partial(shards, mesh.shape["seq"], mesh.shape["tp"]),
        mesh=mesh,
        in_specs=(
            P("seq", None),
            P(),
            P(None, "tp"),
            P("seq", "tp"),
            P("seq", "tp"),
            P("tp", None),
            P(),
            P(),
            P(),
        ),
        out_specs=P(("seq", "tp"), None),
        check_vma=False,
    )
```

```python
import functools
import math

import jax
import jax.numpy as jnp
from jax import lax
from jax.experimental import pallas as pl
from jax.experimental.pallas import tpu as pltpu
from jax.sharding import PartitionSpec as P

HEADS = 32
HD = 128
WINDOW = 4096
SUB = 16
G = 2
KB = 256
KT = 512
NT = 2304
SOFT = 50.0
GAIN = SOFT * math.log2(math.e)
MESH = pl.DeviceIdType.MESH
F32 = jnp.float32
BF16 = jnp.bfloat16


def kernel(
    n, n_tp, kvh, NC,
    starts, counts, hidden, gain_in, wq, key, value, wout, gain_out, out,
    hbuf, wqb, wob, kraw, kt, vb, q0, q2, q4, fs, fr, ns, nr, acc, accd, num, den, numf, denf, rel, sc0, sc1, pw0, pw1, rms, pre_gain, post_gain,
    proj, ra1, pa, ra2, rb1, pb, rb2, res, obuf, att,
    hsem, wqsem, wosem, kvsem, ressem, osem, gsem,
    s1, r1, sn, rn, sf, rf, sF, rF, sN, rN,
    sa1, ta1, sa2, ta2, sb1, tb1, sb2, tb2,
):
    sc = (sc0, sc1)
    pw = (pw0, pw1)
    s = lax.axis_index("seq")
    t = lax.axis_index("tp")
    odd = lax.rem(s, 2)
    partner = s + 1 - 2 * odd
    rows, d = hidden.shape
    ctx = key.shape[0]
    sub = rows // (NC * n_tp)
    chunk = rows // NC
    tall = 2 * chunk
    owned = rows // n_tp
    NF = NC // G
    has_prev = s >= 2
    has_next = s + 2 < n
    has_far = s + 4 < n

    barrier = pltpu.get_barrier_semaphore()
    pl.semaphore_signal(barrier, inc=1, device_id=(partner, t), device_id_type=MESH)
    for k in range(1, n_tp):
        pl.semaphore_signal(barrier, inc=1, device_id=(s, lax.rem(t + k, n_tp)), device_id_type=MESH)

    @pl.when(has_prev)
    def _():
        pl.semaphore_signal(barrier, inc=1, device_id=(s - 2, t), device_id_type=MESH)

    @pl.when(has_next)
    def _():
        pl.semaphore_signal(barrier, inc=1, device_id=(s + 2, t), device_id_type=MESH)

    def h_copy(c, b):
        return pltpu.make_async_copy(
            hidden.at[pl.ds(pl.multiple_of(b * owned + c * sub, sub), sub)], hbuf.at[c, b], hsem.at[c, b])

    def wq_copy(h):
        return pltpu.make_async_copy(
            wq.at[:, pl.ds(pl.multiple_of(h * 2 * HD, 2 * HD), 2 * HD)], wqb.at[h], wqsem.at[h])

    def cols(h):
        return pl.ds(pl.multiple_of(h * HD, HD), HD)

    def kv_local(h):
        return [
            pltpu.make_async_copy(src.at[:, cols(h)], dst.at[0, h], kvsem.at[h, j])
            for j, (src, dst) in enumerate(((key, kraw), (value, vb)))
        ]

    gains = [
        pltpu.make_async_copy(src, dst.at[0], gsem.at[i])
        for i, (src, dst) in enumerate(((gain_in, pre_gain), (gain_out, post_gain)))
    ]
    for cp in gains:
        cp.start()
    for c in range(2):
        for b in range(n_tp):
            h_copy(c, b).start()
    for h in range(kvh):
        wq_copy(h).start()

    def kv_partner(h):
        return [
            pltpu.make_async_remote_copy(
                src.at[:, cols(h)], dst.at[1, h], s1.at[h, j], r1.at[h, j],
                device_id=(partner, t), device_id_type=MESH)
            for j, (src, dst) in enumerate(((key, kraw), (value, vb)))
        ]

    def along(src, dst, send, recv, to):
        def make(c):
            return pltpu.make_async_remote_copy(
                src.at[c], dst.at[c], send.at[c], recv.at[c],
                device_id=(to, t), device_id_type=MESH)
        return make

    q_near = along(q0, q2, sn, rn, s - 2)
    q_far = along(q2, q4, sf, rf, s - 2)
    p_far = along(fs, fr, sF, rF, s + 2)
    p_near = along(ns, nr, sN, rN, s + 2)

    nx = 2
    ny = n_tp // nx
    half = d // 2
    x_own = lax.rem(t, nx)
    y_own = lax.div(t, nx)
    left = pl.ds(0, half)
    right = pl.ds(half, half)

    def remote(src, dst, send, recv, to):
        return pltpu.make_async_remote_copy(
            src, dst, send, recv, device_id=(s, to), device_id_type=MESH)

    def first_phase(c):
        copies = []
        for k in range(1, nx):
            xt = lax.rem(x_own + k, nx)
            copies.append(remote(
                proj.at[c, :, xt, :, :, left], ra1.at[c, k - 1], sa1.at[c, k - 1], ta1.at[c, k - 1],
                y_own * nx + xt))
        for k in range(1, ny):
            yt = lax.rem(y_own + k, ny)
            copies.append(remote(
                proj.at[c, yt, :, :, :, right], rb1.at[c, k - 1], sb1.at[c, k - 1], tb1.at[c, k - 1],
                yt * nx + x_own))
        return copies

    def second_phase(c):
        copies = []
        for k in range(1, ny):
            yt = lax.rem(y_own + k, ny)
            copies.append(remote(
                pa.at[c, yt], ra2.at[c, k - 1], sa2.at[c, k - 1], ta2.at[c, k - 1],
                yt * nx + x_own))
        for k in range(1, nx):
            xt = lax.rem(x_own + k, nx)
            copies.append(remote(
                pb.at[c, xt], rb2.at[c, k - 1], sb2.at[c, k - 1], tb2.at[c, k - 1],
                y_own * nx + xt))
        return copies

    wo_copy = pltpu.make_async_copy(wout, wob, wosem)
    res_copy = pltpu.make_async_copy(
        hidden.at[pl.ds(pl.multiple_of(t * owned, owned), owned)], res, ressem)

    shape = (2, n_tp, sub, KB)
    rel[...] = (
        lax.broadcasted_iota(jnp.int32, shape, 3)
        - lax.broadcasted_iota(jnp.int32, shape, 1) * owned
        - lax.broadcasted_iota(jnp.int32, shape, 2)
    ).reshape(tall, KB)

    @pl.when(s < 2)
    def _():
        fr[...] = jnp.zeros_like(fr)
        nr[...] = jnp.zeros_like(nr)

    def queries(c0, first):
        def arrive(i, carry):
            h_copy(c0 + i // n_tp, i % n_tp).wait()
            return carry

        lax.fori_loop(0, 2 * n_tp, arrive, 0)

        def scale(i, carry):
            x = hbuf[c0 + i // n_tp, i % n_tp].astype(F32)
            r = lax.rsqrt(jnp.mean(x * x, axis=-1, keepdims=True) + 0.1)
            rms[i] = jnp.broadcast_to(r, (sub, HD))
            return carry

        lax.fori_loop(0, 2 * n_tp, scale, 0, unroll=4)
        if first:
            for cp in gains:
                cp.wait()

        def norm(i, carry):
            c = c0 + i // n_tp
            b = i % n_tp
            r = rms[i]
            for k in range(0, d, HD):
                x = hbuf[c, b, :, k:k + HD].astype(F32)
                hbuf[c, b, :, k:k + HD] = (x * r * pre_gain[:, k:k + HD]).astype(BF16)
            return carry

        lax.fori_loop(0, 2 * n_tp, norm, 0)
        if first:
            pl.semaphore_wait(
                barrier, n_tp + jnp.where(has_prev, 1, 0) + jnp.where(has_next, 1, 0))
            for h in range(kvh):
                for cp in kv_local(h):
                    cp.start()
            for h in range(kvh):
                for cp in kv_partner(h):
                    cp.start()
            for c in range(2, NC):
                for b in range(n_tp):
                    h_copy(c, b).start()

        def project(h, carry):
            if first:
                wq_copy(h).wait()
            x = hbuf[pl.ds(c0, 2)].reshape(2 * chunk, d)
            y = jnp.dot(x, wqb[h], preferred_element_type=F32) * ((d // HEADS) ** -0.5 / SOFT)
            y = y.astype(BF16)
            for i in range(2):
                q0[c0 + i, h, 0:chunk] = y[i * chunk:(i + 1) * chunk, :HD]
                q0[c0 + i, h, chunk:tall] = y[i * chunk:(i + 1) * chunk, HD:]
            return carry

        lax.fori_loop(0, kvh, project, 0, unroll=1 if first else 2)

    queries(0, True)
    @pl.when(has_prev)
    def _():
        q_near(0).start()
        q_near(1).start()

    def turn(src):
        def body(h, carry):
            for cp in (kv_local(h) if src == 0 else kv_partner(h)):
                if src == 0:
                    cp.wait()
                else:
                    cp.wait_recv()
            kt[src, h] = kraw[src, h].T
            return carry

        lax.fori_loop(0, kvh, body, 0)

    wo_copy.start()
    res_copy.start()
    turn(0)
    queries(2, False)
    turn(1)

    off_own = starts[s] - s * ctx
    s_far = jnp.minimum(s + 4, n - 1)
    off_far = starts[s_far] - s_far * ctx + 4 * ctx - WINDOW
    fill0 = counts[s]
    fill1 = counts[partner]
    lane = lax.broadcasted_iota(jnp.int32, (1, KB), 1)

    def unit(*parts):
        tiles = []
        for q, c, sources, num, den in parts:
            for h in range(kvh):
                spans = [(src, mode, i) for src, mode in sources for i in range(0, ctx, KT)]
                sums = [None, None]
                for j, (src, mode, i) in enumerate(spans):
                    tiles.append((q, c, num, den, h, src, mode, i, sums, j == len(spans) - 1))

        def scores(j, b):
            q, c, num, den, h, src, mode, i, sums, last = tiles[j]
            sc[j % 2][:, b:b + KB] = jnp.dot(
                q[c, h], kt[src, h, :, i + b:i + b + KB], preferred_element_type=F32)

        def weights(j, b):
            q, c, num, den, h, src, mode, i, sums, last = tiles[j]
            fill = fill1 if src else fill0
            at = i + b
            p = jnp.exp2(jnp.tanh(sc[j % 2][:, b:b + KB]) * GAIN)
            if mode == 1:
                p = jnp.where(rel[...] <= off_own + c * sub - at, p, 0.0)
            elif mode == 2:
                ok = (rel[...] > off_far + c * sub - at) & (lane < fill - at)
                p = jnp.where(ok, p, 0.0)
            else:
                p = jnp.where(lane < fill - at, p, 0.0)
            for k in range(0, KB, HD):
                part = p[:, k:k + HD]
                sums[0] = part if sums[0] is None else sums[0] + part
            pw[j % 2][:, b:b + KB] = p.astype(BF16)
            if last and b == KT - KB:
                den[h] = sums[0]

        def values(j, b):
            q, c, num, den, h, src, mode, i, sums, last = tiles[j]
            a = jnp.dot(
                pw[j % 2][:, b:b + KB], vb[src, h, i + b:i + b + KB], preferred_element_type=F32)
            sums[1] = a if sums[1] is None else sums[1] + a
            if last and b == KT - KB:
                num[h] = sums[1]

        count = len(tiles)
        for k in range(count + 2):
            for b in range(0, KT, KB):
                if k < count:
                    scores(k, b)
                if 0 <= k - 1 < count:
                    weights(k - 1, b)
                if 0 <= k - 2:
                    values(k - 2, b)

    blocks = tall // HD
    lanes = lax.broadcasted_iota(jnp.int32, (tall, HD), 1)

    def received(src, c):
        parts = []
        for i in range(blocks):
            at = kvh * tall + 16 * i
            pair = src[c, at:at + 16].astype(F32)
            parts.append(pair[0:8] + pair[8:16])
        return parts[0] if blocks == 1 else jnp.concatenate(parts, axis=1)

    def emit(c, num, den, dst, extra):
        pack = jnp.zeros((tall, HD), F32)
        for h in range(kvh):
            pack = jnp.where(lanes == h, jnp.sum(den[h], axis=-1, keepdims=True), pack)
        dens = pack.T[0:8]
        if extra is not None:
            dens += received(extra, c)
        hi = dens.astype(BF16).astype(F32)
        both = jnp.concatenate([hi, dens - hi], axis=0).astype(BF16)
        for i in range(blocks):
            at = kvh * tall + 16 * i
            dst[c, at:at + 16] = both[:, i * HD:(i + 1) * HD]
        for h in range(kvh):
            x = num[h]
            if extra is not None:
                x += extra[c, h * tall:(h + 1) * tall].astype(F32)
            dst[c, h * tall:(h + 1) * tall] = x.astype(BF16)

    def relay(c):
        @pl.when(has_next)
        def _():
            q_near(c).wait_recv()

        @pl.when(has_next & has_prev)
        def _():
            q_far(c).start()

    def far_part(c, even):
        return q4, c, [(0, 2), (1, 0)] if even else [(0, 2)], numf, denf

    def near_part(c):
        return q2, c, [(0, 0), (1, 0)], num, den

    def own_part(c, even):
        return q0, c, [(0, 1)] if even else [(0, 1), (1, 0)], acc.at[c], accd.at[c]

    def by_parity(body):
        @pl.when(odd == 0)
        def _():
            body(True)

        @pl.when(odd == 1)
        def _():
            body(False)

    def send_far(c):
        emit(c, numf, denf, fs, None)
        p_far(c).start()

    def send_near(c):
        @pl.when(has_prev)
        def _():
            p_far(c).wait_recv()

        emit(c, num, den, ns, fr)
        p_near(c).start()

    def finish(f):
        for z in range(G):
            c = f * G + z

            @pl.when(has_prev)
            def _():
                p_near(c).wait_recv()

            dens = received(nr, c)
            dens = jnp.concatenate([dens, jnp.zeros((HD - 8, tall), F32)], axis=0).T
            for h in range(kvh):
                total = jnp.sum(accd[c, h], axis=-1, keepdims=True) + dens[:, h:h + 1]
                top = acc[c, h] + nr[c, h * tall:(h + 1) * tall].astype(F32)
                a = (top * (1.0 / total)).astype(BF16)
                for g in range(2):
                    at = (2 * h + g) * HD
                    att[z * chunk:(z + 1) * chunk, at:at + HD] = a[g * chunk:(g + 1) * chunk]

        def column(i, inner):
            cs = pl.ds(pl.multiple_of(i * NT, NT), NT)
            y = jnp.dot(att[...], wob[:, cs], preferred_element_type=F32).astype(BF16)
            for z in range(G):
                proj[f, :, :, z, :, cs] = y[z * chunk:(z + 1) * chunk].reshape(ny, nx, sub, NT)
            return inner

        lax.fori_loop(0, d // NT, column, 0)
        for cp in first_phase(f):
            cp.start()

    def middle(c):
        for cp in first_phase(c):
            cp.wait_recv()
        for y in range(ny):
            part = proj[c, y, x_own, :, :, 0:half].astype(F32)
            for k in range(1, nx):
                part += ra1[c, k - 1, y].astype(F32)
            pa[c, y] = part.astype(BF16)
        for x in range(nx):
            part = proj[c, y_own, x, :, :, half:d].astype(F32)
            for k in range(1, ny):
                part += rb1[c, k - 1, x].astype(F32)
            pb[c, x] = part.astype(BF16)
        for cp in second_phase(c):
            cp.start()

    def out_copy(c):
        return pltpu.make_async_copy(
            obuf.at[c], out.at[pl.ds(pl.multiple_of(c * G * sub, G * sub), G * sub)], osem.at[c])

    def close(c):
        for cp in second_phase(c):
            cp.wait_recv()
        lo = pa[c, y_own].astype(F32)
        for k in range(1, ny):
            lo += ra2[c, k - 1].astype(F32)
        hi = pb[c, x_own].astype(F32)
        for k in range(1, nx):
            hi += rb2[c, k - 1].astype(F32)
        lo = lo.reshape(G * sub, half)
        hi = hi.reshape(G * sub, half)
        squares = jnp.sum(lo * lo, axis=-1, keepdims=True) + jnp.sum(hi * hi, axis=-1, keepdims=True)
        scale = lax.rsqrt(squares / d + 0.1)
        span = pl.ds(pl.multiple_of(c * G * sub, G * sub), G * sub)
        for v, at in ((lo, slice(0, half)), (hi, slice(half, d))):
            r = res[span, at].astype(F32)
            obuf[c, :, at] = (r + v * scale * post_gain[:, at]).astype(BF16)
        out_copy(c).start()

    wo_copy.wait()
    res_copy.wait()

    def step(k, carry):
        full = has_far & (k >= jnp.where(has_prev, 2, 1)) & (k < NC)

        kn = k - jnp.where(has_prev, 2, 1)

        @pl.when(has_prev & (k >= 0) & (k + 2 < NC))
        def _():
            q_near(k + 2).start()

        @pl.when((k >= 0) & (k < NC) & jnp.logical_not(full))
        def _():
            by_parity(lambda even: unit(own_part(k, even)))

        @pl.when(has_far & (k >= 1) & (k <= NC))
        def _():
            q_far(k - 1).wait_recv()

        @pl.when(full)
        def _():
            by_parity(lambda even: unit(far_part(k - 1, even), near_part(kn), own_part(k, even)))

        @pl.when(has_far & (k >= 1) & (k <= NC) & jnp.logical_not(full))
        def _():
            by_parity(lambda even: unit(far_part(k - 1, even)))

        @pl.when(has_far & (k >= 1) & (k <= NC))
        def _():
            send_far(k - 1)

        @pl.when(k + 1 < NC)
        def _():
            relay(k + 1)

        @pl.when(has_next & (kn >= 0) & (kn < NC) & jnp.logical_not(full))
        def _():
            unit(near_part(kn))

        @pl.when(has_next & (kn >= 0) & (kn < NC))
        def _():
            send_near(kn)

        @pl.when((k >= 1) & (lax.rem(k, 2) == 1) & (k + 3 < NC))
        def _():
            queries(k + 3, False)

        @pl.when((k >= G + 2) & (lax.rem(k - 2, G) == 0))
        def _():
            finish((k - G - 2) // G)

        @pl.when((k >= G + 4) & (lax.rem(k - 4, G) == 0))
        def _():
            middle((k - G - 4) // G)

        @pl.when((k >= 2 * G + 4) & (lax.rem(k - 4, G) == 0))
        def _():
            close((k - 2 * G - 4) // G)

        return carry

    lax.fori_loop(-1, NC + 3, step, 0)
    rest = [(G * f + 2 * G + 4, 0, f) for f in range(NF)] + [(G * f + G + 4, 1, f) for f in range(NF)]
    for at, kind, f in sorted(rest):
        if at >= NC + 3:
            (close, middle)[kind](f)

    def drain(h, carry):
        for cp in kv_partner(h):
            cp.wait_send()
        return carry

    lax.fori_loop(0, kvh, drain, 0)

    def drain_chunks(c, carry):
        @pl.when(has_prev)
        def _():
            q_near(c).wait_send()

        @pl.when(has_next & has_prev)
        def _():
            q_far(c).wait_send()

        @pl.when(has_far)
        def _():
            p_far(c).wait_send()

        @pl.when(has_next)
        def _():
            p_near(c).wait_send()

        return carry

    lax.fori_loop(0, NC, drain_chunks, 0)

    def drain_out(c, carry):
        for cp in first_phase(c) + second_phase(c):
            cp.wait_send()
        out_copy(c).wait()
        return carry

    lax.fori_loop(0, NF, drain_out, 0)


def shards(n, n_tp, hidden_in, pre_gain, w_query, key_cache, value_cache, w_out, post_gain, starts, counts):
    rows, d = hidden_in.shape
    ctx, kvw = key_cache.shape
    kvh = kvw // HD
    sub = SUB
    NC = rows // (n_tp * sub)
    NF = NC // G
    chunk = rows // NC
    tall = 2 * chunk
    nx, ny, half = 2, n_tp // 2, d // 2
    dma = pltpu.SemaphoreType.DMA
    kv = pltpu.VMEM((2, kvh, ctx, HD), BF16)
    queries = pltpu.VMEM((NC, kvh, tall, HD), BF16)
    partial = pltpu.VMEM((NC, kvh * tall + 16 * (tall // HD), HD), BF16)
    any_spec = pl.BlockSpec(memory_space=pl.ANY)
    smem_spec = pl.BlockSpec(memory_space=pltpu.SMEM)
    return pl.pallas_call(
        functools.partial(kernel, n, n_tp, kvh, NC),
        out_shape=jax.ShapeDtypeStruct((rows // n_tp, d), BF16),
        in_specs=[smem_spec, smem_spec] + [any_spec] * 7,
        out_specs=any_spec,
        scratch_shapes=[
            pltpu.VMEM((NC, n_tp, sub, d), BF16),
            pltpu.VMEM((kvh, d, 2 * HD), BF16),
            pltpu.VMEM(w_out.shape, BF16),
            kv,
            pltpu.VMEM((2, kvh, HD, ctx), BF16),
            kv,
            queries, queries, queries,
            partial, partial, partial, partial,
            pltpu.VMEM((NC, kvh, tall, HD), F32),
            pltpu.VMEM((NC, kvh, tall, HD), F32),
            pltpu.VMEM((kvh, tall, HD), F32),
            pltpu.VMEM((kvh, tall, HD), F32),
            pltpu.VMEM((kvh, tall, HD), F32),
            pltpu.VMEM((kvh, tall, HD), F32),
            pltpu.VMEM((tall, KB), jnp.int32),
            pltpu.VMEM((tall, KT), F32), pltpu.VMEM((tall, KT), F32),
            pltpu.VMEM((tall, KT), BF16), pltpu.VMEM((tall, KT), BF16),
            pltpu.VMEM((2 * n_tp, sub, HD), F32),
            pltpu.VMEM((1, d), F32), pltpu.VMEM((1, d), F32),
            pltpu.VMEM((NF, ny, nx, G, sub, d), BF16),
            pltpu.VMEM((NF, nx - 1, ny, G, sub, half), BF16),
            pltpu.VMEM((NF, ny, G, sub, half), BF16),
            pltpu.VMEM((NF, ny - 1, G, sub, half), BF16),
            pltpu.VMEM((NF, ny - 1, nx, G, sub, half), BF16),
            pltpu.VMEM((NF, nx, G, sub, half), BF16),
            pltpu.VMEM((NF, nx - 1, G, sub, half), BF16),
            pltpu.VMEM((rows // n_tp, d), BF16),
            pltpu.VMEM((NF, G * sub, d), BF16),
            pltpu.VMEM((G * chunk, w_out.shape[0]), BF16),
            dma((NC, n_tp)), dma((kvh,)), dma, dma((kvh, 2)), dma, dma((NF,)), dma((2,)),
            dma((kvh, 2)), dma((kvh, 2)),
            dma((NC,)), dma((NC,)), dma((NC,)), dma((NC,)),
            dma((NC,)), dma((NC,)), dma((NC,)), dma((NC,)),
            dma((NF, nx - 1)), dma((NF, nx - 1)), dma((NF, ny - 1)), dma((NF, ny - 1)),
            dma((NF, ny - 1)), dma((NF, ny - 1)), dma((NF, nx - 1)), dma((NF, nx - 1)),
        ],
        compiler_params=pltpu.CompilerParams(
            collective_id=0, has_side_effects=True, vmem_limit_bytes=67_000_000),
        name="attention_block",
    )(starts, counts, hidden_in, pre_gain, w_query, key_cache, value_cache, w_out, post_gain)


def solution(mesh):
    return jax.shard_map(
        functools.partial(shards, mesh.shape["seq"], mesh.shape["tp"]),
        mesh=mesh,
        in_specs=(
            P("seq", None),
            P(),
            P(None, "tp"),
            P("seq", "tp"),
            P("seq", "tp"),
            P("tp", None),
            P(),
            P(),
            P(),
        ),
        out_specs=P(("seq", "tp"), None),
        check_vma=False,
    )
```

```python
import functools
import math

import jax
import jax.numpy as jnp
from jax import lax
from jax.experimental import pallas as pl
from jax.experimental.pallas import tpu as pltpu
from jax.sharding import PartitionSpec as P

HEADS = 32
HD = 128
WINDOW = 4096
SUB = 16
KB = 256
UP = 1
KT = 512
NT = 2304
SOFT = 50.0
GAIN = SOFT * math.log2(math.e)
MESH = pl.DeviceIdType.MESH
F32 = jnp.float32
BF16 = jnp.bfloat16


def kernel(
    n, n_tp, kvh, NC,
    starts, counts, hidden, gain_in, wq, key, value, wout, gain_out, out,
    hbuf, wqb, wob, kraw, kt, vb, kx, ktx, vx, q0, q2, q4, fs, fr, ns, nr, acc, accd, num, den, numf, denf, rel, sc0, sc1, pw0, pw1, rms, pre_gain, post_gain,
    proj, ra1, pa, ra2, rb1, pb, rb2, res, obuf, att,
    hsem, wqsem, wosem, kvsem, ressem, osem, gsem,
    s1, r1, su, ru, sr, rr, sn, rn, sf, rf, sF, rF, sN, rN,
    sa1, ta1, sa2, ta2, sb1, tb1, sb2, tb2,
):
    sc = (sc0, sc1)
    pw = (pw0, pw1)
    s = lax.axis_index("seq")
    t = lax.axis_index("tp")
    odd = lax.rem(s, 2)
    partner = s + 1 - 2 * odd
    rows, d = hidden.shape
    ctx = key.shape[0]
    sub = rows // (NC * n_tp)
    chunk = rows // NC
    tall = 2 * chunk
    owned = rows // n_tp
    has_prev = s >= 2
    has_next = s + 2 < n
    has_far = s + 4 < n

    barrier = pltpu.get_barrier_semaphore()
    pl.semaphore_signal(barrier, inc=1, device_id=(partner, t), device_id_type=MESH)
    for k in range(1, n_tp):
        pl.semaphore_signal(barrier, inc=1, device_id=(s, lax.rem(t + k, n_tp)), device_id_type=MESH)

    @pl.when(has_prev)
    def _():
        pl.semaphore_signal(barrier, inc=1, device_id=(s - 2, t), device_id_type=MESH)

    @pl.when(has_next)
    def _():
        pl.semaphore_signal(barrier, inc=1, device_id=(s + 2, t), device_id_type=MESH)

    def h_copy(c, b):
        return pltpu.make_async_copy(
            hidden.at[pl.ds(pl.multiple_of(b * owned + c * sub, sub), sub)], hbuf.at[c, b], hsem.at[c, b])

    def wq_copy(h):
        return pltpu.make_async_copy(
            wq.at[:, pl.ds(pl.multiple_of(h * 2 * HD, 2 * HD), 2 * HD)], wqb.at[h], wqsem.at[h])

    def cols(h):
        return pl.ds(pl.multiple_of(h * HD, HD), HD)

    def kv_local(h):
        return [
            pltpu.make_async_copy(src.at[:, cols(h)], dst.at[0, h], kvsem.at[h, j])
            for j, (src, dst) in enumerate(((key, kraw), (value, vb)))
        ]

    gains = [
        pltpu.make_async_copy(src, dst.at[0], gsem.at[i])
        for i, (src, dst) in enumerate(((gain_in, pre_gain), (gain_out, post_gain)))
    ]
    for cp in gains:
        cp.start()
    for c in range(2):
        for b in range(n_tp):
            h_copy(c, b).start()
    for h in range(kvh):
        wq_copy(h).start()

    def kv_partner(h):
        return [
            pltpu.make_async_remote_copy(
                src.at[:, cols(h)], dst.at[1, h], s1.at[h, j], r1.at[h, j],
                device_id=(partner, t), device_id_type=MESH)
            for j, (src, dst) in enumerate(((key, kraw), (value, vb)))
        ]

    def along(src, dst, send, recv, to, first=0):
        span = pl.ds(first, src.shape[1] - first)

        def make(c):
            return pltpu.make_async_remote_copy(
                src.at[c, span], dst.at[c, span], send.at[c], recv.at[c],
                device_id=(to, t), device_id_type=MESH)
        return make

    def kv_up(h):
        return [
            pltpu.make_async_remote_copy(
                src.at[:, cols(h)], dst.at[0, h], su.at[h, j], ru.at[h, j],
                device_id=(s + 2, t), device_id_type=MESH)
            for j, (src, dst) in enumerate(((key, kx), (value, vx)))
        ]

    def kv_across(h):
        return [
            pltpu.make_async_remote_copy(
                ref.at[0, h], ref.at[1, h], sr.at[h, j], rr.at[h, j],
                device_id=(partner, t), device_id_type=MESH)
            for j, ref in enumerate((kx, vx))
        ]

    q_near = along(q0, q2, sn, rn, s - 2)
    q_far = along(q2, q4, sf, rf, s - 2, UP)
    p_far = along(fs, fr, sF, rF, s + 2, UP * tall)
    p_near = along(ns, nr, sN, rN, s + 2)

    nx = 2
    ny = n_tp // nx
    half = d // 2
    x_own = lax.rem(t, nx)
    y_own = lax.div(t, nx)
    left = pl.ds(0, half)
    right = pl.ds(half, half)

    def remote(src, dst, send, recv, to):
        return pltpu.make_async_remote_copy(
            src, dst, send, recv, device_id=(s, to), device_id_type=MESH)

    def first_phase(c, count):
        span = pl.ds(c, count)
        copies = []
        for k in range(1, nx):
            xt = lax.rem(x_own + k, nx)
            copies.append(remote(
                proj.at[span, :, xt, :, left], ra1.at[k - 1, span], sa1.at[c, k - 1], ta1.at[c, k - 1],
                y_own * nx + xt))
        for k in range(1, ny):
            yt = lax.rem(y_own + k, ny)
            copies.append(remote(
                proj.at[span, yt, :, :, right], rb1.at[k - 1, span], sb1.at[c, k - 1], tb1.at[c, k - 1],
                yt * nx + x_own))
        return copies

    def second_phase(c, count):
        span = pl.ds(c, count)
        copies = []
        for k in range(1, ny):
            yt = lax.rem(y_own + k, ny)
            copies.append(remote(
                pa.at[span, yt], ra2.at[k - 1, span], sa2.at[c, k - 1], ta2.at[c, k - 1],
                yt * nx + x_own))
        for k in range(1, nx):
            xt = lax.rem(x_own + k, nx)
            copies.append(remote(
                pb.at[span, xt], rb2.at[k - 1, span], sb2.at[c, k - 1], tb2.at[c, k - 1],
                y_own * nx + xt))
        return copies

    wo_copy = pltpu.make_async_copy(wout, wob, wosem)
    res_copy = pltpu.make_async_copy(
        hidden.at[pl.ds(pl.multiple_of(t * owned, owned), owned)], res, ressem)

    shape = (2, n_tp, sub, KB)
    rel[...] = (
        lax.broadcasted_iota(jnp.int32, shape, 3)
        - lax.broadcasted_iota(jnp.int32, shape, 1) * owned
        - lax.broadcasted_iota(jnp.int32, shape, 2)
    ).reshape(tall, KB)

    @pl.when(s < 2)
    def _():
        fr[...] = jnp.zeros_like(fr)
        ktx[...] = jnp.zeros_like(ktx)
        vx[...] = jnp.zeros_like(vx)
        nr[...] = jnp.zeros_like(nr)

    def queries(c0, first):
        def arrive(i, carry):
            h_copy(c0 + i // n_tp, i % n_tp).wait()
            return carry

        lax.fori_loop(0, 2 * n_tp, arrive, 0)

        def scale(i, carry):
            x = hbuf[c0 + i // n_tp, i % n_tp].astype(F32)
            r = lax.rsqrt(jnp.mean(x * x, axis=-1, keepdims=True) + 0.1)
            rms[i] = jnp.broadcast_to(r, (sub, HD))
            return carry

        lax.fori_loop(0, 2 * n_tp, scale, 0, unroll=4)
        if first:
            for cp in gains:
                cp.wait()

        def norm(i, carry):
            c = c0 + i // n_tp
            b = i % n_tp
            r = rms[i]
            for k in range(0, d, HD):
                x = hbuf[c, b, :, k:k + HD].astype(F32)
                hbuf[c, b, :, k:k + HD] = (x * r * pre_gain[:, k:k + HD]).astype(BF16)
            return carry

        lax.fori_loop(0, 2 * n_tp, norm, 0)
        if first:
            pl.semaphore_wait(
                barrier, n_tp + jnp.where(has_prev, 1, 0) + jnp.where(has_next, 1, 0))
            @pl.when(has_next)
            def _():
                for h in range(UP):
                    for cp in kv_up(h):
                        cp.start()

            for h in range(kvh):
                for cp in kv_local(h):
                    cp.start()
            for h in range(kvh):
                for cp in kv_partner(h):
                    cp.start()
            for c in range(2, NC):
                for b in range(n_tp):
                    h_copy(c, b).start()

        def project(h, carry):
            if first:
                wq_copy(h).wait()
            x = hbuf[pl.ds(c0, 2)].reshape(2 * chunk, d)
            y = jnp.dot(x, wqb[h], preferred_element_type=F32) * ((d // HEADS) ** -0.5 / SOFT)
            y = y.astype(BF16)
            for i in range(2):
                q0[c0 + i, h, 0:chunk] = y[i * chunk:(i + 1) * chunk, :HD]
                q0[c0 + i, h, chunk:tall] = y[i * chunk:(i + 1) * chunk, HD:]
            return carry

        lax.fori_loop(0, kvh, project, 0, unroll=1 if first else 2)

    queries(0, True)
    @pl.when(has_prev)
    def _():
        q_near(0).start()
        q_near(1).start()

    def turn(src):
        def body(h, carry):
            for cp in (kv_local(h) if src == 0 else kv_partner(h)):
                if src == 0:
                    cp.wait()
                else:
                    cp.wait_recv()
            kt[src, h] = kraw[src, h].T
            return carry

        lax.fori_loop(0, kvh, body, 0)

    wo_copy.start()
    res_copy.start()
    turn(0)
    queries(2, False)
    turn(1)

    off_own = starts[s] - s * ctx
    s_far = jnp.minimum(s + 4, n - 1)
    off_far = starts[s_far] - s_far * ctx + 4 * ctx - WINDOW
    s_next = jnp.minimum(s + 2, n - 1)
    off_next = starts[s_next] - s_next * ctx + 4 * ctx - WINDOW
    fills = (
        counts[s],
        counts[partner],
        jnp.where(has_prev, counts[jnp.maximum(s - 2, 0)], 0),
        jnp.where(has_prev, counts[jnp.maximum(s - 1, 0)], 0),
    )
    lane = lax.broadcasted_iota(jnp.int32, (1, KB), 1)

    def unit(*parts):
        tiles = []
        for q, c, sources, num, den in parts:
            for h in range(kvh):
                spans = [(src, mode, i) for src, mode in sources(h) for i in range(0, ctx, KT)]
                sums = [None, None]
                for j, (src, mode, i) in enumerate(spans):
                    tiles.append((q, c, num, den, h, src, mode, i, sums, j == len(spans) - 1))

        def scores(j, b):
            q, c, num, den, h, src, mode, i, sums, last = tiles[j]
            k = kt[src, h, :, i + b:i + b + KB] if src < 2 else ktx[src - 2, h, :, i + b:i + b + KB]
            sc[j % 2][:, b:b + KB] = jnp.dot(q[c, h], k, preferred_element_type=F32)

        def weights(j, b):
            q, c, num, den, h, src, mode, i, sums, last = tiles[j]
            fill = fills[src]
            at = i + b
            p = jnp.exp2(jnp.tanh(sc[j % 2][:, b:b + KB]) * GAIN)
            if mode == 1:
                p = jnp.where(rel[...] <= off_own + c * sub - at, p, 0.0)
            elif mode >= 2:
                off = off_far if mode == 2 else off_next
                ok = (rel[...] > off + c * sub - at) & (lane < fill - at)
                p = jnp.where(ok, p, 0.0)
            else:
                p = jnp.where(lane < fill - at, p, 0.0)
            for k in range(0, KB, HD):
                part = p[:, k:k + HD]
                sums[0] = part if sums[0] is None else sums[0] + part
            pw[j % 2][:, b:b + KB] = p.astype(BF16)
            if last and b == KT - KB:
                den[h] = sums[0]

        def values(j, b):
            q, c, num, den, h, src, mode, i, sums, last = tiles[j]
            v = vb[src, h, i + b:i + b + KB] if src < 2 else vx[src - 2, h, i + b:i + b + KB]
            a = jnp.dot(pw[j % 2][:, b:b + KB], v, preferred_element_type=F32)
            sums[1] = a if sums[1] is None else sums[1] + a
            if last and b == KT - KB:
                num[h] = sums[1]

        count = len(tiles)
        for k in range(count + 2):
            for b in range(0, KT, KB):
                if k < count:
                    scores(k, b)
                if 0 <= k - 1 < count:
                    weights(k - 1, b)
                if 0 <= k - 2:
                    values(k - 2, b)

    blocks = tall // HD
    lanes = lax.broadcasted_iota(jnp.int32, (tall, HD), 1)

    def received(src, c):
        parts = []
        for i in range(blocks):
            at = kvh * tall + 16 * i
            pair = src[c, at:at + 16].astype(F32)
            parts.append(pair[0:8] + pair[8:16])
        return parts[0] if blocks == 1 else jnp.concatenate(parts, axis=1)

    def emit(c, num, den, dst, extra, least):
        pack = jnp.zeros((tall, HD), F32)
        for h in range(least, kvh):
            pack = jnp.where(lanes == h, jnp.sum(den[h], axis=-1, keepdims=True), pack)
        dens = pack.T[0:8]
        if extra is not None:
            dens += received(extra, c)
        hi = dens.astype(BF16).astype(F32)
        both = jnp.concatenate([hi, dens - hi], axis=0).astype(BF16)
        for i in range(blocks):
            at = kvh * tall + 16 * i
            dst[c, at:at + 16] = both[:, i * HD:(i + 1) * HD]
        for h in range(least, kvh):
            x = num[h]
            if extra is not None and h >= UP:
                x += extra[c, h * tall:(h + 1) * tall].astype(F32)
            dst[c, h * tall:(h + 1) * tall] = x.astype(BF16)

    def relay(c):
        @pl.when(has_next)
        def _():
            q_near(c).wait_recv()

        @pl.when(has_next & has_prev)
        def _():
            q_far(c).start()

    def far_part(c, even):
        def sources(h):
            if h < UP:
                return []
            return [(0, 2), (1, 0)] if even else [(0, 2)]
        return q4, c, sources, numf, denf

    def near_part(c, even):
        def sources(h):
            return [(2, 3), (3 if even else 1, 0)] if h < UP else [(0, 0), (1, 0)]
        return q2, c, sources, num, den

    def own_part(c, even):
        def sources(h):
            if h < UP:
                return [(0, 1), (3 if even else 1, 0), (2, 0)]
            return [(0, 1)] if even else [(0, 1), (1, 0)]
        return q0, c, sources, acc.at[c], accd.at[c]

    def by_parity(body):
        @pl.when(odd == 0)
        def _():
            body(True)

        @pl.when(odd == 1)
        def _():
            body(False)

    def send_far(c):
        emit(c, numf, denf, fs, None, UP)
        p_far(c).start()

    def send_near(c):
        @pl.when(has_prev)
        def _():
            p_far(c).wait_recv()

        emit(c, num, den, ns, fr, 0)
        p_near(c).start()

    def finish(c0, count):
        for z in range(count):
            c = c0 + z

            @pl.when(has_prev)
            def _():
                p_near(c).wait_recv()

            dens = received(nr, c)
            dens = jnp.concatenate([dens, jnp.zeros((HD - 8, tall), F32)], axis=0).T
            for h in range(kvh):
                total = jnp.sum(accd[c, h], axis=-1, keepdims=True) + dens[:, h:h + 1]
                top = acc[c, h] + nr[c, h * tall:(h + 1) * tall].astype(F32)
                a = (top * (1.0 / total)).astype(BF16)
                for g in range(2):
                    at = (2 * h + g) * HD
                    att[z * chunk:(z + 1) * chunk, at:at + HD] = a[g * chunk:(g + 1) * chunk]

        def column(i, inner):
            cs = pl.ds(pl.multiple_of(i * NT, NT), NT)
            y = jnp.dot(
                att[0:count * chunk], wob[:, cs], preferred_element_type=F32).astype(BF16)
            for z in range(count):
                proj[c0 + z, :, :, :, cs] = y[z * chunk:(z + 1) * chunk].reshape(ny, nx, sub, NT)
            return inner

        lax.fori_loop(0, d // NT, column, 0)
        for cp in first_phase(c0, count):
            cp.start()

    def middle(c0, count):
        for cp in first_phase(c0, count):
            cp.wait_recv()
        for z in range(count):
            c = c0 + z
            for y in range(ny):
                part = proj[c, y, x_own, :, 0:half].astype(F32)
                for k in range(1, nx):
                    part += ra1[k - 1, c, y].astype(F32)
                pa[c, y] = part.astype(BF16)
            for x in range(nx):
                part = proj[c, y_own, x, :, half:d].astype(F32)
                for k in range(1, ny):
                    part += rb1[k - 1, c, x].astype(F32)
                pb[c, x] = part.astype(BF16)
        for cp in second_phase(c0, count):
            cp.start()

    def out_copy(c):
        return pltpu.make_async_copy(
            obuf.at[c], out.at[pl.ds(pl.multiple_of(c * sub, sub), sub)], osem.at[c])

    def close(c0, count):
        for cp in second_phase(c0, count):
            cp.wait_recv()
        for z in range(count):
            c = c0 + z
            lo = pa[c, y_own].astype(F32)
            for k in range(1, ny):
                lo += ra2[k - 1, c].astype(F32)
            hi = pb[c, x_own].astype(F32)
            for k in range(1, nx):
                hi += rb2[k - 1, c].astype(F32)
            squares = jnp.sum(lo * lo, axis=-1, keepdims=True) + jnp.sum(hi * hi, axis=-1, keepdims=True)
            scale = lax.rsqrt(squares / d + 0.1)
            span = pl.ds(pl.multiple_of(c * sub, sub), sub)
            for v, at in ((lo, slice(0, half)), (hi, slice(half, d))):
                r = res[span, at].astype(F32)
                obuf[c, :, at] = (r + v * scale * post_gain[:, at]).astype(BF16)
            out_copy(c).start()

    wo_copy.wait()
    res_copy.wait()

    def lift():
        for h in range(UP):
            for cp in kv_up(h):
                cp.wait_recv()

        @pl.when(odd == 1)
        def _():
            for h in range(UP):
                for cp in kv_across(h):
                    cp.start()

        for h in range(UP):
            ktx[0, h] = kx[0, h].T

        @pl.when(odd == 0)
        def _():
            for h in range(UP):
                for cp in kv_across(h):
                    cp.wait_recv()
                ktx[1, h] = kx[1, h].T

    def step(k, carry):
        kn = k - jnp.where(has_prev, 2, 1)
        nearby = has_next & (kn >= 0) & (kn < NC)
        middling = (k >= 1) & (k <= NC)
        full = has_far & nearby & middling

        @pl.when(has_prev & (k >= 0) & (k + 2 < NC))
        def _():
            q_near(k + 2).start()

        @pl.when(has_far & middling)
        def _():
            q_far(k - 1).wait_recv()

        @pl.when(full)
        def _():
            by_parity(lambda even: unit(
                far_part(k - 1, even), near_part(kn, even), own_part(k - 1, even)))

        @pl.when(has_far & middling & jnp.logical_not(full))
        def _():
            by_parity(lambda even: unit(far_part(k - 1, even)))

        @pl.when(has_far & middling)
        def _():
            send_far(k - 1)

        @pl.when(k + 1 < NC)
        def _():
            relay(k + 1)

        @pl.when((k >= 0) & (2 * k + 4 < NC))
        def _():
            queries(2 * k + 4, False)

        @pl.when(has_prev & (k == 1))
        def _():
            lift()

        @pl.when(nearby & jnp.logical_not(full))
        def _():
            by_parity(lambda even: unit(near_part(kn, even)))

        @pl.when(nearby)
        def _():
            send_near(kn)

        @pl.when(middling & jnp.logical_not(full))
        def _():
            by_parity(lambda even: unit(own_part(k - 1, even)))

        @pl.when(k == 3)
        def _():
            finish(0, 1)

        paired = (lax.rem(k, 2) == 1) & (k <= NC + 1)

        @pl.when(paired & (k >= 5))
        def _():
            finish(k - 4, 2)

        @pl.when(k == NC + 2)
        def _():
            finish(NC - 1, 1)

        @pl.when(k == 4)
        def _():
            middle(0, 1)

        @pl.when(paired & (k >= 7))
        def _():
            middle(k - 6, 2)

        @pl.when(k == 6)
        def _():
            close(0, 1)

        @pl.when(paired & (k >= 9))
        def _():
            close(k - 8, 2)

        return carry

    lax.fori_loop(-1, NC + 3, step, 0)
    middle(NC - 3, 2)
    if NC > 4:
        close(NC - 5, 2)
    middle(NC - 1, 1)
    close(NC - 3, 2)
    close(NC - 1, 1)

    @pl.when(has_next)
    def _():
        for h in range(UP):
            for cp in kv_up(h):
                cp.wait_send()

    @pl.when(has_prev & (odd == 1))
    def _():
        for h in range(UP):
            for cp in kv_across(h):
                cp.wait_send()

    def drain(h, carry):
        for cp in kv_partner(h):
            cp.wait_send()
        return carry

    lax.fori_loop(0, kvh, drain, 0)

    def drain_chunks(c, carry):
        @pl.when(has_prev)
        def _():
            q_near(c).wait_send()

        @pl.when(has_next & has_prev)
        def _():
            q_far(c).wait_send()

        @pl.when(has_far)
        def _():
            p_far(c).wait_send()

        @pl.when(has_next)
        def _():
            p_near(c).wait_send()

        return carry

    lax.fori_loop(0, NC, drain_chunks, 0)

    def drain_phases(c, count):
        for cp in first_phase(c, count) + second_phase(c, count):
            cp.wait_send()

    def drain_pairs(g, carry):
        drain_phases(2 * g + 1, 2)
        return carry

    def drain_out(c, carry):
        out_copy(c).wait()
        return carry

    drain_phases(0, 1)
    lax.fori_loop(0, NC // 2 - 1, drain_pairs, 0)
    drain_phases(NC - 1, 1)
    lax.fori_loop(0, NC, drain_out, 0)


def shards(n, n_tp, hidden_in, pre_gain, w_query, key_cache, value_cache, w_out, post_gain, starts, counts):
    rows, d = hidden_in.shape
    ctx, kvw = key_cache.shape
    kvh = kvw // HD
    sub = SUB
    NC = rows // (n_tp * sub)
    chunk = rows // NC
    tall = 2 * chunk
    nx, ny, half = 2, n_tp // 2, d // 2
    dma = pltpu.SemaphoreType.DMA
    kv = pltpu.VMEM((2, kvh, ctx, HD), BF16)
    queries = pltpu.VMEM((NC, kvh, tall, HD), BF16)
    partial = pltpu.VMEM((NC, kvh * tall + 16 * (tall // HD), HD), BF16)
    any_spec = pl.BlockSpec(memory_space=pl.ANY)
    smem_spec = pl.BlockSpec(memory_space=pltpu.SMEM)
    return pl.pallas_call(
        functools.partial(kernel, n, n_tp, kvh, NC),
        out_shape=jax.ShapeDtypeStruct((rows // n_tp, d), BF16),
        in_specs=[smem_spec, smem_spec] + [any_spec] * 7,
        out_specs=any_spec,
        scratch_shapes=[
            pltpu.VMEM((NC, n_tp, sub, d), BF16),
            pltpu.VMEM((kvh, d, 2 * HD), BF16),
            pltpu.VMEM(w_out.shape, BF16),
            kv,
            pltpu.VMEM((2, kvh, HD, ctx), BF16),
            kv,
            pltpu.VMEM((2, UP, ctx, HD), BF16),
            pltpu.VMEM((2, UP, HD, ctx), BF16),
            pltpu.VMEM((2, UP, ctx, HD), BF16),
            queries, queries, queries,
            partial, partial, partial, partial,
            pltpu.VMEM((NC, kvh, tall, HD), F32),
            pltpu.VMEM((NC, kvh, tall, HD), F32),
            pltpu.VMEM((kvh, tall, HD), F32),
            pltpu.VMEM((kvh, tall, HD), F32),
            pltpu.VMEM((kvh, tall, HD), F32),
            pltpu.VMEM((kvh, tall, HD), F32),
            pltpu.VMEM((tall, KB), jnp.int32),
            pltpu.VMEM((tall, KT), F32), pltpu.VMEM((tall, KT), F32),
            pltpu.VMEM((tall, KT), BF16), pltpu.VMEM((tall, KT), BF16),
            pltpu.VMEM((2 * n_tp, sub, HD), F32),
            pltpu.VMEM((1, d), F32), pltpu.VMEM((1, d), F32),
            pltpu.VMEM((NC, ny, nx, sub, d), BF16),
            pltpu.VMEM((nx - 1, NC, ny, sub, half), BF16),
            pltpu.VMEM((NC, ny, sub, half), BF16),
            pltpu.VMEM((ny - 1, NC, sub, half), BF16),
            pltpu.VMEM((ny - 1, NC, nx, sub, half), BF16),
            pltpu.VMEM((NC, nx, sub, half), BF16),
            pltpu.VMEM((nx - 1, NC, sub, half), BF16),
            pltpu.VMEM((rows // n_tp, d), BF16),
            pltpu.VMEM((NC, sub, d), BF16),
            pltpu.VMEM((2 * chunk, w_out.shape[0]), BF16),
            dma((NC, n_tp)), dma((kvh,)), dma, dma((kvh, 2)), dma, dma((NC,)), dma((2,)),
            dma((kvh, 2)), dma((kvh, 2)),
            dma((UP, 2)), dma((UP, 2)), dma((UP, 2)), dma((UP, 2)),
            dma((NC,)), dma((NC,)), dma((NC,)), dma((NC,)),
            dma((NC,)), dma((NC,)), dma((NC,)), dma((NC,)),
            dma((NC, nx - 1)), dma((NC, nx - 1)), dma((NC, ny - 1)), dma((NC, ny - 1)),
            dma((NC, ny - 1)), dma((NC, ny - 1)), dma((NC, nx - 1)), dma((NC, nx - 1)),
        ],
        compiler_params=pltpu.CompilerParams(
            collective_id=0, has_side_effects=True, vmem_limit_bytes=67_000_000),
        name="attention_block",
    )(starts, counts, hidden_in, pre_gain, w_query, key_cache, value_cache, w_out, post_gain)


def solution(mesh):
    return jax.shard_map(
        functools.partial(shards, mesh.shape["seq"], mesh.shape["tp"]),
        mesh=mesh,
        in_specs=(
            P("seq", None),
            P(),
            P(None, "tp"),
            P("seq", "tp"),
            P("seq", "tp"),
            P("tp", None),
            P(),
            P(),
            P(),
        ),
        out_specs=P(("seq", "tp"), None),
        check_vma=False,
    )
```

```python
import functools
import math

import jax
import jax.numpy as jnp
from jax import lax
from jax.experimental import pallas as pl
from jax.experimental.pallas import tpu as pltpu
from jax.sharding import PartitionSpec as P

HEADS = 32
HD = 128
WINDOW = 4096
SUB = 16
KB = 256
UP = 1
KT = 512
NT = 2304
SOFT = 50.0
GAIN = SOFT * math.log2(math.e)
MESH = pl.DeviceIdType.MESH
F32 = jnp.float32
BF16 = jnp.bfloat16


def kernel(
    n, n_tp, kvh, NC,
    starts, counts, hidden, gain_in, wq, key, value, wout, gain_out, out,
    hbuf, wqb, wob, kraw, kt, vb, kx, ktx, vx, q0, q2, q4, fs, fr, ns, nr, acc, accd, num, den, numf, denf, rel, sc0, sc1, pw0, pw1, rms, pre_gain, post_gain,
    proj, ra1, pa, ra2, rb1, pb, rb2, res, obuf, att,
    hsem, wqsem, wosem, kvsem, ressem, osem, gsem,
    s1, r1, su, ru, sr, rr, sn, rn, sf, rf, sF, rF, sN, rN,
    sa1, ta1, sa2, ta2, sb1, tb1, sb2, tb2,
):
    sc = (sc0, sc1)
    pw = (pw0, pw1)
    s = lax.axis_index("seq")
    t = lax.axis_index("tp")
    odd = lax.rem(s, 2)
    partner = s + 1 - 2 * odd
    rows, d = hidden.shape
    ctx = key.shape[0]
    sub = rows // (NC * n_tp)
    chunk = rows // NC
    tall = 2 * chunk
    owned = rows // n_tp
    has_prev = s >= 2
    has_next = s + 2 < n
    has_far = s + 4 < n

    barrier = pltpu.get_barrier_semaphore()
    pl.semaphore_signal(barrier, inc=1, device_id=(partner, t), device_id_type=MESH)
    for k in range(1, n_tp):
        pl.semaphore_signal(barrier, inc=1, device_id=(s, lax.rem(t + k, n_tp)), device_id_type=MESH)

    @pl.when(has_prev)
    def _():
        pl.semaphore_signal(barrier, inc=1, device_id=(s - 2, t), device_id_type=MESH)

    @pl.when(has_next)
    def _():
        pl.semaphore_signal(barrier, inc=1, device_id=(s + 2, t), device_id_type=MESH)

    def h_copy(c, b):
        return pltpu.make_async_copy(
            hidden.at[pl.ds(pl.multiple_of(b * owned + c * sub, sub), sub)], hbuf.at[c, b], hsem.at[c, b])

    def wq_copy(h):
        return pltpu.make_async_copy(
            wq.at[:, pl.ds(pl.multiple_of(h * 2 * HD, 2 * HD), 2 * HD)], wqb.at[h], wqsem.at[h])

    def cols(h):
        return pl.ds(pl.multiple_of(h * HD, HD), HD)

    def kv_local(h):
        return [
            pltpu.make_async_copy(src.at[:, cols(h)], dst.at[0, h], kvsem.at[h, j])
            for j, (src, dst) in enumerate(((key, kraw), (value, vb)))
        ]

    gains = [
        pltpu.make_async_copy(src, dst.at[0], gsem.at[i])
        for i, (src, dst) in enumerate(((gain_in, pre_gain), (gain_out, post_gain)))
    ]
    for cp in gains:
        cp.start()
    for c in range(2):
        for b in range(n_tp):
            h_copy(c, b).start()
    for h in range(kvh):
        wq_copy(h).start()

    def kv_partner(h):
        return [
            pltpu.make_async_remote_copy(
                src.at[:, cols(h)], dst.at[1, h], s1.at[h, j], r1.at[h, j],
                device_id=(partner, t), device_id_type=MESH)
            for j, (src, dst) in enumerate(((key, kraw), (value, vb)))
        ]

    def along(src, dst, send, recv, to, first=0):
        span = pl.ds(first, src.shape[1] - first)

        def make(c):
            return pltpu.make_async_remote_copy(
                src.at[c, span], dst.at[c, span], send.at[c], recv.at[c],
                device_id=(to, t), device_id_type=MESH)
        return make

    def kv_up(h):
        return [
            pltpu.make_async_remote_copy(
                src.at[:, cols(h)], dst.at[0, h], su.at[h, j], ru.at[h, j],
                device_id=(s + 2, t), device_id_type=MESH)
            for j, (src, dst) in enumerate(((key, kx), (value, vx)))
        ]

    def kv_across(h):
        return [
            pltpu.make_async_remote_copy(
                ref.at[0, h], ref.at[1, h], sr.at[h, j], rr.at[h, j],
                device_id=(partner, t), device_id_type=MESH)
            for j, ref in enumerate((kx, vx))
        ]

    q_near = along(q0, q2, sn, rn, s - 2)
    q_far = along(q2, q4, sf, rf, s - 2, UP)
    p_far = along(fs, fr, sF, rF, s + 2, UP * tall)
    p_near = along(ns, nr, sN, rN, s + 2)

    nx = 2
    ny = n_tp // nx
    half = d // 2
    x_own = lax.rem(t, nx)
    y_own = lax.div(t, nx)
    left = pl.ds(0, half)
    right = pl.ds(half, half)

    def remote(src, dst, send, recv, to):
        return pltpu.make_async_remote_copy(
            src, dst, send, recv, device_id=(s, to), device_id_type=MESH)

    def first_phase(c, count):
        span = pl.ds(c, count)
        copies = []
        for k in range(1, nx):
            xt = lax.rem(x_own + k, nx)
            copies.append(remote(
                proj.at[span, :, xt, :, left], ra1.at[k - 1, span], sa1.at[c, k - 1], ta1.at[c, k - 1],
                y_own * nx + xt))
        for k in range(1, ny):
            yt = lax.rem(y_own + k, ny)
            copies.append(remote(
                proj.at[span, yt, :, :, right], rb1.at[k - 1, span], sb1.at[c, k - 1], tb1.at[c, k - 1],
                yt * nx + x_own))
        return copies

    def second_phase(c, count):
        span = pl.ds(c, count)
        copies = []
        for k in range(1, ny):
            yt = lax.rem(y_own + k, ny)
            copies.append(remote(
                pa.at[span, yt], ra2.at[k - 1, span], sa2.at[c, k - 1], ta2.at[c, k - 1],
                yt * nx + x_own))
        for k in range(1, nx):
            xt = lax.rem(x_own + k, nx)
            copies.append(remote(
                pb.at[span, xt], rb2.at[k - 1, span], sb2.at[c, k - 1], tb2.at[c, k - 1],
                y_own * nx + xt))
        return copies

    wo_copy = pltpu.make_async_copy(wout, wob, wosem)
    res_copy = pltpu.make_async_copy(
        hidden.at[pl.ds(pl.multiple_of(t * owned, owned), owned)], res, ressem)

    shape = (2, n_tp, sub, KB)
    rel[...] = (
        lax.broadcasted_iota(jnp.int32, shape, 3)
        - lax.broadcasted_iota(jnp.int32, shape, 1) * owned
        - lax.broadcasted_iota(jnp.int32, shape, 2)
    ).reshape(tall, KB)

    @pl.when(s < 2)
    def _():
        fr[...] = jnp.zeros_like(fr)
        ktx[...] = jnp.zeros_like(ktx)
        vx[...] = jnp.zeros_like(vx)
        nr[...] = jnp.zeros_like(nr)

    def queries(c0, first):
        def arrive(i, carry):
            h_copy(c0 + i // n_tp, i % n_tp).wait()
            return carry

        lax.fori_loop(0, 2 * n_tp, arrive, 0)

        def scale(i, carry):
            x = hbuf[c0 + i // n_tp, i % n_tp].astype(F32)
            r = lax.rsqrt(jnp.mean(x * x, axis=-1, keepdims=True) + 0.1)
            rms[i] = jnp.broadcast_to(r, (sub, HD))
            return carry

        lax.fori_loop(0, 2 * n_tp, scale, 0, unroll=4)
        if first:
            for cp in gains:
                cp.wait()

        def norm(i, carry):
            c = c0 + i // n_tp
            b = i % n_tp
            r = rms[i]
            for k in range(0, d, HD):
                x = hbuf[c, b, :, k:k + HD].astype(F32)
                hbuf[c, b, :, k:k + HD] = (x * r * pre_gain[:, k:k + HD]).astype(BF16)
            return carry

        lax.fori_loop(0, 2 * n_tp, norm, 0)
        if first:
            pl.semaphore_wait(
                barrier, n_tp + jnp.where(has_prev, 1, 0) + jnp.where(has_next, 1, 0))
            @pl.when(has_next)
            def _():
                for h in range(UP):
                    for cp in kv_up(h):
                        cp.start()

            for h in range(kvh):
                for cp in kv_local(h):
                    cp.start()
            for h in range(kvh):
                for cp in kv_partner(h):
                    cp.start()
            for c in range(2, NC):
                for b in range(n_tp):
                    h_copy(c, b).start()

        def project(h, carry):
            if first:
                wq_copy(h).wait()
            x = hbuf[pl.ds(c0, 2)].reshape(2 * chunk, d)
            y = jnp.dot(x, wqb[h], preferred_element_type=F32) * ((d // HEADS) ** -0.5 / SOFT)
            y = y.astype(BF16)
            for i in range(2):
                q0[c0 + i, h, 0:chunk] = y[i * chunk:(i + 1) * chunk, :HD]
                q0[c0 + i, h, chunk:tall] = y[i * chunk:(i + 1) * chunk, HD:]
            return carry

        lax.fori_loop(0, kvh, project, 0, unroll=1 if first else 2)

    queries(0, True)
    @pl.when(has_prev)
    def _():
        q_near(0).start()
        q_near(1).start()

    def turn(src):
        def body(h, carry):
            for cp in (kv_local(h) if src == 0 else kv_partner(h)):
                if src == 0:
                    cp.wait()
                else:
                    cp.wait_recv()
            kt[src, h] = kraw[src, h].T
            return carry

        lax.fori_loop(0, kvh, body, 0)

    wo_copy.start()
    res_copy.start()
    turn(0)
    queries(2, False)
    turn(1)

    off_own = starts[s] - s * ctx
    s_far = jnp.minimum(s + 4, n - 1)
    off_far = starts[s_far] - s_far * ctx + 4 * ctx - WINDOW
    s_next = jnp.minimum(s + 2, n - 1)
    off_next = starts[s_next] - s_next * ctx + 4 * ctx - WINDOW
    fills = (
        counts[s],
        counts[partner],
        jnp.where(has_prev, counts[jnp.maximum(s - 2, 0)], 0),
        jnp.where(has_prev, counts[jnp.maximum(s - 1, 0)], 0),
    )
    lane = lax.broadcasted_iota(jnp.int32, (1, KB), 1)

    def unit(*parts):
        tiles = []
        for q, c, sources, num, den in parts:
            for h in range(kvh):
                spans = [(src, mode, i) for src, mode in sources(h) for i in range(0, ctx, KT)]
                sums = [None, None]
                for j, (src, mode, i) in enumerate(spans):
                    tiles.append((q, c, num, den, h, src, mode, i, sums, j == len(spans) - 1))

        def scores(j, b):
            q, c, num, den, h, src, mode, i, sums, last = tiles[j]
            k = kt[src, h, :, i + b:i + b + KB] if src < 2 else ktx[src - 2, h, :, i + b:i + b + KB]
            sc[j % 2][:, b:b + KB] = jnp.dot(q[c, h], k, preferred_element_type=F32)

        def weights(j, b):
            q, c, num, den, h, src, mode, i, sums, last = tiles[j]
            fill = fills[src]
            at = i + b
            p = jnp.exp2(jnp.tanh(sc[j % 2][:, b:b + KB]) * GAIN)
            if mode == 1:
                p = jnp.where(rel[...] <= off_own + c * sub - at, p, 0.0)
            elif mode >= 2:
                off = off_far if mode == 2 else off_next
                ok = (rel[...] > off + c * sub - at) & (lane < fill - at)
                p = jnp.where(ok, p, 0.0)
            else:
                p = jnp.where(lane < fill - at, p, 0.0)
            for k in range(0, KB, HD):
                part = p[:, k:k + HD]
                sums[0] = part if sums[0] is None else sums[0] + part
            pw[j % 2][:, b:b + KB] = p.astype(BF16)
            if last and b == KT - KB:
                den[h] = sums[0]

        def values(j, b):
            q, c, num, den, h, src, mode, i, sums, last = tiles[j]
            v = vb[src, h, i + b:i + b + KB] if src < 2 else vx[src - 2, h, i + b:i + b + KB]
            a = jnp.dot(pw[j % 2][:, b:b + KB], v, preferred_element_type=F32)
            sums[1] = a if sums[1] is None else sums[1] + a
            if last and b == KT - KB:
                num[h] = sums[1]

        count = len(tiles)
        for k in range(count + 2):
            for b in range(0, KT, KB):
                if k < count:
                    scores(k, b)
                if 0 <= k - 1 < count:
                    weights(k - 1, b)
                if 0 <= k - 2:
                    values(k - 2, b)

    blocks = tall // HD
    lanes = lax.broadcasted_iota(jnp.int32, (tall, HD), 1)

    def received(src, c):
        parts = []
        for i in range(blocks):
            at = kvh * tall + 16 * i
            pair = src[c, at:at + 16].astype(F32)
            parts.append(pair[0:8] + pair[8:16])
        return parts[0] if blocks == 1 else jnp.concatenate(parts, axis=1)

    def emit(c, num, den, dst, extra, least):
        pack = jnp.zeros((tall, HD), F32)
        for h in range(least, kvh):
            pack = jnp.where(lanes == h, jnp.sum(den[h], axis=-1, keepdims=True), pack)
        dens = pack.T[0:8]
        if extra is not None:
            dens += received(extra, c)
        hi = dens.astype(BF16).astype(F32)
        both = jnp.concatenate([hi, dens - hi], axis=0).astype(BF16)
        for i in range(blocks):
            at = kvh * tall + 16 * i
            dst[c, at:at + 16] = both[:, i * HD:(i + 1) * HD]
        for h in range(least, kvh):
            x = num[h]
            if extra is not None and h >= UP:
                x += extra[c, h * tall:(h + 1) * tall].astype(F32)
            dst[c, h * tall:(h + 1) * tall] = x.astype(BF16)

    def relay(c):
        @pl.when(has_next)
        def _():
            q_near(c).wait_recv()

        @pl.when(has_next & has_prev)
        def _():
            q_far(c).start()

    def far_part(c, even):
        def sources(h):
            if h < UP:
                return []
            return [(0, 2), (1, 0)] if even else [(0, 2)]
        return q4, c, sources, numf, denf

    def near_part(c, even):
        def sources(h):
            return [(2, 3), (3 if even else 1, 0)] if h < UP else [(0, 0), (1, 0)]
        return q2, c, sources, num, den

    def own_part(c, even):
        def sources(h):
            if h < UP:
                return [(0, 1), (3 if even else 1, 0), (2, 0)]
            return [(0, 1)] if even else [(0, 1), (1, 0)]
        return q0, c, sources, acc.at[c], accd.at[c]

    def by_parity(body):
        @pl.when(odd == 0)
        def _():
            body(True)

        @pl.when(odd == 1)
        def _():
            body(False)

    def send_far(c):
        emit(c, numf, denf, fs, None, UP)
        p_far(c).start()

    def send_near(c):
        @pl.when(has_prev)
        def _():
            p_far(c).wait_recv()

        emit(c, num, den, ns, fr, 0)
        p_near(c).start()

    def finish(c0, count):
        for z in range(count):
            c = c0 + z

            @pl.when(has_prev)
            def _():
                p_near(c).wait_recv()

            dens = received(nr, c)
            dens = jnp.concatenate([dens, jnp.zeros((HD - 8, tall), F32)], axis=0).T
            for h in range(kvh):
                total = jnp.sum(accd[c, h], axis=-1, keepdims=True) + dens[:, h:h + 1]
                top = acc[c, h] + nr[c, h * tall:(h + 1) * tall].astype(F32)
                a = (top * (1.0 / total)).astype(BF16)
                for g in range(2):
                    at = (2 * h + g) * HD
                    att[z * chunk:(z + 1) * chunk, at:at + HD] = a[g * chunk:(g + 1) * chunk]

        def column(i, inner):
            cs = pl.ds(pl.multiple_of(i * NT, NT), NT)
            y = jnp.dot(
                att[0:count * chunk], wob[:, cs], preferred_element_type=F32).astype(BF16)
            for z in range(count):
                proj[c0 + z, :, :, :, cs] = y[z * chunk:(z + 1) * chunk].reshape(ny, nx, sub, NT)
            return inner

        lax.fori_loop(0, d // NT, column, 0)
        for cp in first_phase(c0, count):
            cp.start()

    def middle(c0, count):
        for cp in first_phase(c0, count):
            cp.wait_recv()
        for z in range(count):
            c = c0 + z
            for y in range(ny):
                part = proj[c, y, x_own, :, 0:half].astype(F32)
                for k in range(1, nx):
                    part += ra1[k - 1, c, y].astype(F32)
                pa[c, y] = part.astype(BF16)
            for x in range(nx):
                part = proj[c, y_own, x, :, half:d].astype(F32)
                for k in range(1, ny):
                    part += rb1[k - 1, c, x].astype(F32)
                pb[c, x] = part.astype(BF16)
        for cp in second_phase(c0, count):
            cp.start()

    def out_copy(c):
        return pltpu.make_async_copy(
            obuf.at[c], out.at[pl.ds(pl.multiple_of(c * sub, sub), sub)], osem.at[c])

    def close(c0, count):
        for cp in second_phase(c0, count):
            cp.wait_recv()
        for z in range(count):
            c = c0 + z
            lo = pa[c, y_own].astype(F32)
            for k in range(1, ny):
                lo += ra2[k - 1, c].astype(F32)
            hi = pb[c, x_own].astype(F32)
            for k in range(1, nx):
                hi += rb2[k - 1, c].astype(F32)
            squares = jnp.sum(lo * lo, axis=-1, keepdims=True) + jnp.sum(hi * hi, axis=-1, keepdims=True)
            scale = lax.rsqrt(squares / d + 0.1)
            span = pl.ds(pl.multiple_of(c * sub, sub), sub)
            for v, at in ((lo, slice(0, half)), (hi, slice(half, d))):
                r = res[span, at].astype(F32)
                obuf[c, :, at] = (r + v * scale * post_gain[:, at]).astype(BF16)
            out_copy(c).start()

    wo_copy.wait()
    res_copy.wait()

    def lift():
        for h in range(UP):
            for cp in kv_up(h):
                cp.wait_recv()

        @pl.when(odd == 1)
        def _():
            for h in range(UP):
                for cp in kv_across(h):
                    cp.start()

        for h in range(UP):
            ktx[0, h] = kx[0, h].T

        @pl.when(odd == 0)
        def _():
            for h in range(UP):
                for cp in kv_across(h):
                    cp.wait_recv()
                ktx[1, h] = kx[1, h].T

    def step(k, carry):
        kn = k - jnp.where(has_prev, 2, 1)
        nearby = has_next & (kn >= 0) & (kn < NC)
        middling = (k >= 1) & (k <= NC)
        full = has_far & nearby & middling

        @pl.when(has_prev & (k >= 0) & (k + 2 < NC))
        def _():
            q_near(k + 2).start()

        @pl.when(has_far & middling)
        def _():
            q_far(k - 1).wait_recv()

        @pl.when(full)
        def _():
            by_parity(lambda even: unit(
                far_part(k - 1, even), near_part(kn, even), own_part(k - 1, even)))

        @pl.when(has_far & middling & jnp.logical_not(full))
        def _():
            by_parity(lambda even: unit(far_part(k - 1, even)))

        @pl.when(has_far & middling)
        def _():
            send_far(k - 1)

        @pl.when(k + 1 < NC)
        def _():
            relay(k + 1)

        @pl.when((k >= 0) & (2 * k + 4 < NC))
        def _():
            queries(2 * k + 4, False)

        @pl.when(has_prev & (k == 1))
        def _():
            lift()

        @pl.when(nearby & jnp.logical_not(full))
        def _():
            by_parity(lambda even: unit(near_part(kn, even)))

        @pl.when(middling & jnp.logical_not(full))
        def _():
            by_parity(lambda even: unit(own_part(k - 1, even)))

        @pl.when(nearby)
        def _():
            send_near(kn)

        @pl.when(k == 3)
        def _():
            finish(0, 1)

        paired = (lax.rem(k, 2) == 1) & (k <= NC + 1)

        @pl.when(paired & (k >= 5))
        def _():
            finish(k - 4, 2)

        @pl.when(k == NC + 2)
        def _():
            finish(NC - 1, 1)

        @pl.when(k == 4)
        def _():
            middle(0, 1)

        @pl.when(paired & (k >= 7))
        def _():
            middle(k - 6, 2)

        @pl.when(k == 6)
        def _():
            close(0, 1)

        @pl.when(paired & (k >= 9))
        def _():
            close(k - 8, 2)

        return carry

    lax.fori_loop(-1, NC + 3, step, 0)
    middle(NC - 3, 2)
    if NC > 4:
        close(NC - 5, 2)
    middle(NC - 1, 1)
    close(NC - 3, 2)
    close(NC - 1, 1)

    @pl.when(has_next)
    def _():
        for h in range(UP):
            for cp in kv_up(h):
                cp.wait_send()

    @pl.when(has_prev & (odd == 1))
    def _():
        for h in range(UP):
            for cp in kv_across(h):
                cp.wait_send()

    def drain(h, carry):
        for cp in kv_partner(h):
            cp.wait_send()
        return carry

    lax.fori_loop(0, kvh, drain, 0)

    def drain_chunks(c, carry):
        @pl.when(has_prev)
        def _():
            q_near(c).wait_send()

        @pl.when(has_next & has_prev)
        def _():
            q_far(c).wait_send()

        @pl.when(has_far)
        def _():
            p_far(c).wait_send()

        @pl.when(has_next)
        def _():
            p_near(c).wait_send()

        return carry

    lax.fori_loop(0, NC, drain_chunks, 0)

    def drain_phases(c, count):
        for cp in first_phase(c, count) + second_phase(c, count):
            cp.wait_send()

    def drain_pairs(g, carry):
        drain_phases(2 * g + 1, 2)
        return carry

    def drain_out(c, carry):
        out_copy(c).wait()
        return carry

    drain_phases(0, 1)
    lax.fori_loop(0, NC // 2 - 1, drain_pairs, 0)
    drain_phases(NC - 1, 1)
    lax.fori_loop(0, NC, drain_out, 0)


def shards(n, n_tp, hidden_in, pre_gain, w_query, key_cache, value_cache, w_out, post_gain, starts, counts):
    rows, d = hidden_in.shape
    ctx, kvw = key_cache.shape
    kvh = kvw // HD
    sub = SUB
    NC = rows // (n_tp * sub)
    chunk = rows // NC
    tall = 2 * chunk
    nx, ny, half = 2, n_tp // 2, d // 2
    dma = pltpu.SemaphoreType.DMA
    kv = pltpu.VMEM((2, kvh, ctx, HD), BF16)
    queries = pltpu.VMEM((NC, kvh, tall, HD), BF16)
    partial = pltpu.VMEM((NC, kvh * tall + 16 * (tall // HD), HD), BF16)
    any_spec = pl.BlockSpec(memory_space=pl.ANY)
    smem_spec = pl.BlockSpec(memory_space=pltpu.SMEM)
    return pl.pallas_call(
        functools.partial(kernel, n, n_tp, kvh, NC),
        out_shape=jax.ShapeDtypeStruct((rows // n_tp, d), BF16),
        in_specs=[smem_spec, smem_spec] + [any_spec] * 7,
        out_specs=any_spec,
        scratch_shapes=[
            pltpu.VMEM((NC, n_tp, sub, d), BF16),
            pltpu.VMEM((kvh, d, 2 * HD), BF16),
            pltpu.VMEM(w_out.shape, BF16),
            kv,
            pltpu.VMEM((2, kvh, HD, ctx), BF16),
            kv,
            pltpu.VMEM((2, UP, ctx, HD), BF16),
            pltpu.VMEM((2, UP, HD, ctx), BF16),
            pltpu.VMEM((2, UP, ctx, HD), BF16),
            queries, queries, queries,
            partial, partial, partial, partial,
            pltpu.VMEM((NC, kvh, tall, HD), F32),
            pltpu.VMEM((NC, kvh, tall, HD), F32),
            pltpu.VMEM((kvh, tall, HD), F32),
            pltpu.VMEM((kvh, tall, HD), F32),
            pltpu.VMEM((kvh, tall, HD), F32),
            pltpu.VMEM((kvh, tall, HD), F32),
            pltpu.VMEM((tall, KB), jnp.int32),
            pltpu.VMEM((tall, KT), F32), pltpu.VMEM((tall, KT), F32),
            pltpu.VMEM((tall, KT), BF16), pltpu.VMEM((tall, KT), BF16),
            pltpu.VMEM((2 * n_tp, sub, HD), F32),
            pltpu.VMEM((1, d), F32), pltpu.VMEM((1, d), F32),
            pltpu.VMEM((NC, ny, nx, sub, d), BF16),
            pltpu.VMEM((nx - 1, NC, ny, sub, half), BF16),
            pltpu.VMEM((NC, ny, sub, half), BF16),
            pltpu.VMEM((ny - 1, NC, sub, half), BF16),
            pltpu.VMEM((ny - 1, NC, nx, sub, half), BF16),
            pltpu.VMEM((NC, nx, sub, half), BF16),
            pltpu.VMEM((nx - 1, NC, sub, half), BF16),
            pltpu.VMEM((rows // n_tp, d), BF16),
            pltpu.VMEM((NC, sub, d), BF16),
            pltpu.VMEM((2 * chunk, w_out.shape[0]), BF16),
            dma((NC, n_tp)), dma((kvh,)), dma, dma((kvh, 2)), dma, dma((NC,)), dma((2,)),
            dma((kvh, 2)), dma((kvh, 2)),
            dma((UP, 2)), dma((UP, 2)), dma((UP, 2)), dma((UP, 2)),
            dma((NC,)), dma((NC,)), dma((NC,)), dma((NC,)),
            dma((NC,)), dma((NC,)), dma((NC,)), dma((NC,)),
            dma((NC, nx - 1)), dma((NC, nx - 1)), dma((NC, ny - 1)), dma((NC, ny - 1)),
            dma((NC, ny - 1)), dma((NC, ny - 1)), dma((NC, nx - 1)), dma((NC, nx - 1)),
        ],
        compiler_params=pltpu.CompilerParams(
            collective_id=0, has_side_effects=True, vmem_limit_bytes=67_000_000),
        name="attention_block",
    )(starts, counts, hidden_in, pre_gain, w_query, key_cache, value_cache, w_out, post_gain)


def solution(mesh):
    return jax.shard_map(
        functools.partial(shards, mesh.shape["seq"], mesh.shape["tp"]),
        mesh=mesh,
        in_specs=(
            P("seq", None),
            P(),
            P(None, "tp"),
            P("seq", "tp"),
            P("seq", "tp"),
            P("tp", None),
            P(),
            P(),
            P(),
        ),
        out_specs=P(("seq", "tp"), None),
        check_vma=False,
    )
```
